32 devices in a mesh: dp: 2 (over x), sx: 4 (over z), sy: 4 (over y, core).
Axes of the slice: x: 2, y: 2, z: 4, core: 2. Of those that a mesh axis runs over, the one named last changes fastest.
Arguments:
- act_in: bfloat16 [32, 384, 64, 256], P('dp', 'sy', 'sx'), parts along dimension 0
- norm_first: bfloat16 [2, 256], replicated
- w_first: bfloat16 [3, 3, 256, 128], replicated
- w_short: bfloat16 [256, 128], replicated
- norm_rest: bfloat16 [6, 2, 128], replicated
- w_rest: bfloat16 [5, 3, 3, 128, 128], replicated
- bias_rest: bfloat16 [7, 128], replicated
- w_out: bfloat16 [3, 3, 128, 3], replicated
- bias_out: bfloat16 [3], replicated
Outputs:
- output: float32 [32, 384, 64, 3], P('dp', 'sy', 'sx'), parts along dimension 0
There are 2 independent parts. The reference program is written for one: setup_inputs(seed, part) draws one part's arguments, and reference() takes and returns one part's arrays. A program takes and returns all parts, laid end to end along the dimension named above; an argument that names none is the same for every part.
All inputs are finite; a program needn't handle non-finite values.
Results may differ from the reference program's by a relative error of at most 0.00891096.
Values are sent between devices in bfloat16 or wider.
A program may use at most 1 GiB of HBM per device.

```python
import math
import jax
import jax.numpy as jnp
from jax import lax

SAMPLES = 16
IMG_H = 384
IMG_W = 64
IN_CH = 256
MID_CH = 128
OUT_CH = 3
GROUPS = 32
GN_EPS = 1e-6


def normal_weight(key, shape, fan_in):
    return (jax.random.normal(key, shape, jnp.float32) * fan_in ** -0.5).astype(jnp.bfloat16)


def norm_params(key, layer_count, chan_count):
    gain_key, shift_key = jax.random.split(key)
    gains = 1.0 + 0.25 * jax.random.normal(gain_key, (layer_count, chan_count), jnp.float32)
    shifts = 0.25 * jax.random.normal(shift_key, (layer_count, chan_count), jnp.float32)
    return jnp.stack([gains, shifts], axis=1).astype(jnp.bfloat16)


def setup_inputs(seed: int = 0, part: int = 0) -> dict:
    base_key = jax.random.key(seed)
    act_keys = jax.random.split(jax.random.fold_in(base_key, part), 6)
    weight_keys = jax.random.split(base_key, 8)
    wave_count = 3
    base_noise = jax.random.normal(act_keys[0], (SAMPLES, IMG_H, IMG_W, IN_CH), jnp.float32)
    wave_amp = jax.random.normal(act_keys[1], (SAMPLES, wave_count, 1, IN_CH), jnp.float32)
    row_freq = jax.random.uniform(act_keys[2], (SAMPLES, wave_count, 1, 1), jnp.float32, 0.5, 2.5)
    col_freq = jax.random.uniform(act_keys[3], (SAMPLES, wave_count, 1, 1), jnp.float32, 0.5, 2.5)
    row_phase = jax.random.uniform(act_keys[4], (SAMPLES, wave_count, 1, IN_CH), jnp.float32, 0.0, 2.0 * math.pi)
    col_phase = jax.random.uniform(act_keys[5], (SAMPLES, wave_count, 1, IN_CH), jnp.float32, 0.0, 2.0 * math.pi)
    row_pos = (jnp.arange(IMG_H, dtype=jnp.float32) / IMG_H)[:, None]
    col_pos = (jnp.arange(IMG_W, dtype=jnp.float32) / IMG_W)[:, None]
    row_wave = wave_amp * jnp.cos(2.0 * math.pi * row_freq * row_pos + row_phase)
    col_wave = jnp.cos(2.0 * math.pi * col_freq * col_pos + col_phase)
    smooth_field = jnp.einsum("skhc,skwc->shwc", row_wave, col_wave)
    act_in = (0.7 * base_noise + smooth_field).astype(jnp.bfloat16)
    return {
        "act_in": act_in,
        "norm_first": norm_params(weight_keys[0], 1, IN_CH)[0],
        "w_first": normal_weight(weight_keys[1], (3, 3, IN_CH, MID_CH), 9 * IN_CH),
        "w_short": normal_weight(weight_keys[2], (IN_CH, MID_CH), IN_CH),
        "norm_rest": norm_params(weight_keys[3], 6, MID_CH),
        "w_rest": normal_weight(weight_keys[4], (5, 3, 3, MID_CH, MID_CH), 9 * MID_CH),
        "bias_rest": (0.3 * jax.random.normal(weight_keys[5], (7, MID_CH), jnp.float32)).astype(jnp.bfloat16),
        "w_out": normal_weight(weight_keys[6], (3, 3, MID_CH, OUT_CH), 9 * MID_CH),
        "bias_out": (0.3 * jax.random.normal(weight_keys[7], (OUT_CH,), jnp.float32)).astype(jnp.bfloat16),
    }


def group_norm_act(act_map, norm_pair):
    num_rows, num_cols, channels = act_map.shape
    per_group = channels // GROUPS
    group_count = num_rows * num_cols * per_group
    sum_one = jnp.sum(act_map, axis=(0, 1), dtype=jnp.float32).reshape(GROUPS, per_group).sum(axis=1)
    sum_two = jnp.sum(jnp.square(act_map.astype(jnp.float32)), axis=(0, 1)).reshape(GROUPS, per_group).sum(axis=1)
    group_mean = sum_one / group_count
    inv_std = lax.rsqrt(sum_two / group_count - group_mean * group_mean + GN_EPS)
    chan_scale = jnp.repeat(inv_std, per_group) * norm_pair[0].astype(jnp.float32)
    chan_shift = norm_pair[1].astype(jnp.float32) - jnp.repeat(group_mean, per_group) * chan_scale
    return jax.nn.silu(act_map.astype(jnp.float32) * chan_scale + chan_shift).astype(jnp.bfloat16)


def conv_three(act_map, kernel):
    num_rows, num_cols, in_chans = act_map.shape
    padded = jnp.pad(act_map, ((1, 1), (1, 1), (0, 0)))
    accum_sum = jnp.zeros((num_rows * num_cols, kernel.shape[3]), jnp.float32)
    for row_off in range(3):
        for col_off in range(3):
            window = padded[row_off:row_off + num_rows, col_off:col_off + num_cols].reshape(num_rows * num_cols, in_chans)
            accum_sum = accum_sum + jnp.dot(window, kernel[row_off, col_off], preferred_element_type=jnp.float32)
    return accum_sum.reshape(num_rows, num_cols, kernel.shape[3])


def reference(act_in, norm_first, w_first, w_short, norm_rest, w_rest, bias_rest, w_out, bias_out):
    bias_rows = bias_rest.astype(jnp.float32)

    def decode_sample(sample):
        num_rows, num_cols, in_chans = sample.shape
        mid_act = (conv_three(group_norm_act(sample, norm_first), w_first) + bias_rows[0]).astype(jnp.bfloat16)
        skip_path = jnp.dot(sample.reshape(num_rows * num_cols, in_chans), w_short, preferred_element_type=jnp.float32).reshape(num_rows, num_cols, -1) + bias_rows[6]
        hidden = (conv_three(group_norm_act(mid_act, norm_rest[0]), w_rest[0]) + bias_rows[1] + skip_path).astype(jnp.bfloat16)
        for res_index in range(1, 3):
            first_at = 2 * res_index - 1
            mid_act = (conv_three(group_norm_act(hidden, norm_rest[first_at]), w_rest[first_at]) + bias_rows[first_at + 1]).astype(jnp.bfloat16)
            hidden = (conv_three(group_norm_act(mid_act, norm_rest[first_at + 1]), w_rest[first_at + 1]) + bias_rows[first_at + 2] + hidden.astype(jnp.float32)).astype(jnp.bfloat16)
        return conv_three(group_norm_act(hidden, norm_rest[5]), w_out) + bias_out.astype(jnp.float32)

    return lax.map(decode_sample, act_in)
```

```python
import functools

import jax
import jax.numpy as jnp
from jax import lax
from jax.experimental import pallas as pl
from jax.experimental.pallas import tpu as pltpu
from jax.sharding import PartitionSpec as P

GROUPS = 32
GN_EPS = 1e-6
MESH = pl.DeviceIdType.MESH
F32 = jnp.float32
LANES = 128
WIDE = 256
SUB = 16
BF16 = jnp.bfloat16
SLAB = 48
BLOCK = 8
STEPS = SLAB // BLOCK
CHUNK = 4
DEPTH = 3
CHUNKS = SLAB // CHUNK


def exact_rows(values):
    high = values.astype(BF16).astype(F32)
    rest = values - high
    mid = rest.astype(BF16).astype(F32)
    low = rest - mid
    return jnp.concatenate([high, mid, low, jnp.zeros_like(low)], axis=0).astype(BF16)


def exact_dot(values, ones):
    out = jnp.dot(exact_rows(values), ones, preferred_element_type=F32)
    return (out[0:8] + out[8:SUB]) + out[SUB:24]


def group_matrix(channels, transposed):
    per_group = channels // GROUPS
    shape = (LANES, 2 * channels) if transposed else (2 * channels, LANES)
    chan = lax.broadcasted_iota(jnp.int32, shape, 1 if transposed else 0)
    lane = lax.broadcasted_iota(jnp.int32, shape, 0 if transposed else 1)
    target = jnp.where(chan < channels, chan // per_group, GROUPS + (chan - channels) // per_group)
    return jnp.where(target == lane, 1.0, 0.0).astype(BF16)


def kernel(rows_n, cols_n, act_in, norm_first, w_first, w_short, norm_rest, w_rest, bias_rest, w_out, image,
           stage, raw_a, raw_t, raw_h, act_a, act_t, wf, ws, wr, wo, perm, sum_a, sum_t, cast_a, cast_t,
           col_a, row_a, cor_a, col_t, row_t, cor_t, slots,
           in_sem, wt_sem, col_send, col_recv, row_send, row_recv, cor_send, cor_recv, stat_send, stat_recv):
    peers = rows_n * cols_n
    my_x = lax.axis_index("sx")
    my_y = lax.axis_index("sy")
    me = my_x * rows_n + my_y
    has_side = (my_x > 0, my_x < cols_n - 1)
    has_end = (my_y > 0, my_y < rows_n - 1)
    count = float(rows_n * cols_n * 2 * SLAB * SUB)

    def at(dx, dy):
        return {"sx": my_x + dx, "sy": my_y + dy}

    def peer(index):
        return {"sx": index // rows_n, "sy": lax.rem(index, rows_n)}

    def col_copy(raw, col, par, g, side, start, size):
        src = raw.at[g, pl.ds(start, size), 0 if side == 0 else 7, side]
        dst = col.at[par, g, 1 - side, pl.ds(start, size)]
        return pltpu.make_async_remote_copy(src, dst, col_send.at[par, g, side], col_recv.at[par, g, 1 - side], device_id=at(2 * side - 1, 0), device_id_type=MESH)

    def row_copy(raw, row, par, g, end):
        src = raw.at[g, 0 if end == 0 else SLAB - 1]
        return pltpu.make_async_remote_copy(src, row.at[par, g, 1 - end], row_send.at[par, g, end], row_recv.at[par, g, 1 - end], device_id=at(0, 2 * end - 1), device_id_type=MESH)

    def cor_copy(raw, cor, par, g, end, side):
        src = raw.at[g, 0 if end == 0 else SLAB - 1, 0 if side == 0 else 7, side]
        return pltpu.make_async_remote_copy(src, cor.at[par, g, 1 - end, 1 - side], cor_send.at[par, g, end, side], cor_recv.at[par, g, 1 - end, 1 - side], device_id=at(2 * side - 1, 2 * end - 1), device_id_type=MESH)

    def stat_copy(par, g, offset):
        return pltpu.make_async_remote_copy(slots.at[par, g, me], slots.at[par, g, me], stat_send.at[par, g], stat_recv.at[par, g], device_id=peer(lax.rem(me + offset, peers)), device_id_type=MESH)

    def send_cols(raw, col, par, g, step):
        for side in range(2):
            @pl.when(has_side[side])
            def _():
                col_copy(raw, col, par, g, side, step * BLOCK, BLOCK).start()

    def send_ends(raw, row, cor, par, g):
        for end in range(2):
            @pl.when(has_end[end])
            def _():
                row_copy(raw, row, par, g, end).start()
            for side in range(2):
                @pl.when(jnp.logical_and(has_end[end], has_side[side]))
                def _():
                    cor_copy(raw, cor, par, g, end, side).start()

    def send_sums(par, g, message):
        slots[par, g, me] = message

        def one(offset, carry):
            stat_copy(par, g, offset).start()
            return carry

        lax.fori_loop(1, peers, one, 0)

    def finish_exchange(raw, col, row, cor, par, g):
        for side in range(2):
            @pl.when(has_side[side])
            def _():
                col_copy(raw, col, par, g, side, 0, SLAB).wait_send()
                col_copy(raw, col, par, g, 1 - side, 0, SLAB).wait_recv()
        for end in range(2):
            @pl.when(has_end[end])
            def _():
                row_copy(raw, row, par, g, end).wait_send()
                row_copy(raw, row, par, g, 1 - end).wait_recv()
            for side in range(2):
                @pl.when(jnp.logical_and(has_end[end], has_side[side]))
                def _():
                    cor_copy(raw, cor, par, g, end, side).wait_send()
                    cor_copy(raw, cor, par, g, 1 - end, 1 - side).wait_recv()
        arrived = slots.at[par, g, pl.ds(0, peers - 1)]
        done = pltpu.make_async_remote_copy(arrived, arrived, stat_send.at[par, g], stat_recv.at[par, g], device_id=peer(lax.rem(me + 1, peers)), device_id_type=MESH)
        done.wait_send()
        done.wait_recv()

    def message_of(sum_one, sum_two, ones):
        both = jnp.concatenate([sum_one[0:8] + sum_one[8:SUB], sum_two[0:8] + sum_two[8:SUB]], axis=1)
        return exact_dot(both, ones)

    def half_affine(par, g, spread, norm_pair, channels):
        totals = slots[par, g, 0]
        for index in range(1, peers):
            totals = totals + slots[par, g, index]
        sums = exact_dot(totals, spread)
        inv_count = 1.0 / (count * (channels // GROUPS))
        mean = sums[:, :channels] * inv_count
        inv_std = lax.rsqrt(sums[:, channels:] * inv_count - mean * mean + GN_EPS)
        pair = norm_pair.astype(F32)
        scale = inv_std * pair[0:1]
        shift = pair[1:2] - mean * scale
        scale, shift = scale * 0.5, shift * 0.5
        return jnp.concatenate([scale, scale], axis=0), jnp.concatenate([shift, shift], axis=0)

    def activate(values, scale, shift):
        half = values.astype(F32) * scale + shift
        return half + half * jnp.tanh(half)

    def activation(raw, act, col, row, cor, par, g, scale, shift, block):
        def body(step, carry):
            first = step * block
            out = activate(raw[g, pl.ds(first, block)], scale, shift).astype(BF16)
            act[pl.ds(first + 1, block), 0:8, 1] = out[:, :, 0]
            act[pl.ds(first + 1, block), 1:9, 0] = out[:, :, 1]
            for side in range(2):
                edge = activate(col[par, g, side, pl.ds(first, block)], scale, shift)
                act[pl.ds(first + 1, block), 8 * side, side] = jnp.where(has_side[side], edge, 0.0).astype(BF16)
            return carry

        lax.fori_loop(0, SLAB // block, body, 0)
        for end in range(2):
            keep, other = (slice(8, SUB), slice(0, 8)) if end == 0 else (slice(0, 8), slice(8, SUB))
            dest = 0 if end == 0 else SLAB + 1
            inner = SLAB if end == 0 else 1

            def put(pair_at, which, remote, present):
                mine = act[inner, pair_at, which].astype(F32)
                far = jnp.where(present, remote, 0.0)[..., keep, :]
                near = mine[..., other, :]
                parts = [far, near] if end == 0 else [near, far]
                act[dest, pair_at, which] = jnp.concatenate(parts, axis=-2).astype(BF16)

            line = activate(row[par, g, end], scale, shift)
            put(slice(0, 8), 1, line[:, 0], has_end[end])
            put(slice(1, 9), 0, line[:, 1], has_end[end])
            for side in range(2):
                spot = activate(cor[par, g, end, side], scale, shift)
                put(8 * side, side, spot, jnp.logical_and(has_end[end], has_side[side]))

    def windows(act, first, channels):
        taps = []
        for row_off in range(3):
            for col_off in range(4):
                pair_at = col_off // 2
                taps.append(act[pl.ds(first + row_off, BLOCK), pair_at:pair_at + 8, col_off % 2].reshape(BLOCK * LANES, channels))
        return taps

    def convolve(act, channels, weights, bias, dst, col, row, cor, par, g, extra=None, residual=None):
        bias_pair = jnp.concatenate([bias, bias], axis=1)

        def body(step, carry):
            sum_one, sum_two = carry
            first = step * BLOCK
            taps = windows(act, first, channels)
            if extra is not None:
                taps = taps + extra(first)
            out = jnp.dot(jnp.concatenate(taps, axis=1), weights(), preferred_element_type=F32) + bias_pair
            if residual is not None:
                kept = residual[g, pl.ds(first, BLOCK)].astype(F32)
                kept = jnp.concatenate([kept[:, :, 0], kept[:, :, 1]], axis=-1)
                out = out + kept.reshape(BLOCK * LANES, WIDE)
            rounded = out.astype(BF16)
            wide = rounded.astype(F32).reshape(BLOCK * 8, SUB, WIDE)
            sum_one = sum_one + jnp.sum(wide, axis=0)
            sum_two = sum_two + jnp.sum(wide * wide, axis=0)
            tiles = rounded.reshape(BLOCK, 8, SUB, WIDE)
            dst[g, pl.ds(first, BLOCK), :, 0] = tiles[..., :LANES]
            dst[g, pl.ds(first, BLOCK), :, 1] = tiles[..., LANES:]

            @pl.when(step > 0)
            def _():
                send_cols(dst, col, par, g, step - 1)

            return sum_one, sum_two

        zero = jnp.zeros((SUB, WIDE), F32)
        sum_one, sum_two = lax.fori_loop(0, STEPS, body, (zero, zero))
        send_sums(par, g, message_of(sum_one[:, :LANES] + sum_one[:, LANES:], sum_two[:, :LANES] + sum_two[:, LANES:], sum_t[...]))
        send_cols(dst, col, par, g, STEPS - 1)
        send_ends(dst, row, cor, par, g)

    def input_copy(g, chunk, half):
        index = g * CHUNKS + chunk
        slot = lax.rem(index, DEPTH)
        src = act_in.at[pl.ds(g * 8, 8), pl.ds(half * SLAB + chunk * CHUNK, CHUNK)]
        return pltpu.make_async_copy(src, stage.at[slot, half], in_sem.at[slot, half])

    for early in range(DEPTH):
        for half in range(2):
            input_copy(0, early, half).start()

    barrier = pltpu.get_barrier_semaphore()

    def greet(offset, carry):
        pl.semaphore_signal(barrier, inc=1, device_id=peer(lax.rem(me + offset, peers)), device_id_type=MESH)
        return carry

    lax.fori_loop(1, peers, greet, 0)

    out_row = lax.broadcasted_iota(jnp.int32, (WIDE, WIDE), 0)
    in_row = lax.broadcasted_iota(jnp.int32, (WIDE, WIDE), 1)
    swapped = jnp.logical_and(out_row // SUB == in_row % SUB, out_row % SUB == in_row // SUB)
    perm[...] = jnp.where(swapped, 1.0, 0.0).astype(BF16)
    sum_a[...] = group_matrix(WIDE, False)
    sum_t[...] = group_matrix(LANES, False)
    cast_a[...] = group_matrix(WIDE, True)
    cast_t[...] = group_matrix(LANES, True)
    for tap in range(3):
        wf[tap, 3, :, 0:LANES] = jnp.zeros((WIDE, LANES), BF16)
        wf[tap, 0, :, LANES:WIDE] = jnp.zeros((WIDE, LANES), BF16)
        for layer in range(5):
            wr[layer, tap, 3, :, 0:LANES] = jnp.zeros((LANES, LANES), BF16)
            wr[layer, tap, 0, :, LANES:WIDE] = jnp.zeros((LANES, LANES), BF16)
    ws[0, :, LANES:WIDE] = jnp.zeros((WIDE, LANES), BF16)
    ws[1, :, 0:LANES] = jnp.zeros((WIDE, LANES), BF16)

    def weight_copies():
        copies = []
        for out_col in range(2):
            lanes = pl.ds(out_col * LANES, LANES)
            copies.append(pltpu.make_async_copy(w_first, wf.at[:, pl.ds(out_col, 3), :, lanes], wt_sem.at[0, out_col]))
            copies.append(pltpu.make_async_copy(w_short, ws.at[out_col, :, lanes], wt_sem.at[1, out_col]))
            copies.append(pltpu.make_async_copy(w_rest, wr.at[:, :, pl.ds(out_col, 3), :, lanes], wt_sem.at[2, out_col]))
        return copies

    for copy in weight_copies():
        copy.start()

    blank = jnp.zeros((3, LANES), F32)
    for row_off in range(3):
        for col_off in range(4):
            parts = []
            for out_col in range(2):
                tap = col_off - out_col
                parts.append(w_out[row_off, tap].astype(F32) if 0 <= tap < 3 else blank)
            parts.append(jnp.zeros((10, LANES), F32))
            at_lane = (row_off * 4 + col_off) * LANES
            wo[:, at_lane:at_lane + LANES] = jnp.concatenate(parts, axis=0).astype(BF16)

    def load_group(g, carry):
        def body(chunk, sums):
            sum_one, sum_two = sums
            index = g * CHUNKS + chunk
            slot = lax.rem(index, DEPTH)
            for half in range(2):
                input_copy(g, chunk, half).wait()
            for line in range(CHUNK):
                tile = stage[slot, :, :, line].reshape(WIDE, WIDE)
                out = jnp.dot(perm[...], tile, preferred_element_type=F32)
                cube = out.reshape(SUB, SUB, WIDE)
                sum_one = sum_one + jnp.sum(cube, axis=0)
                sum_two = sum_two + jnp.sum(cube * cube, axis=0)
                raw_a[g, chunk * CHUNK + line] = out.astype(BF16).reshape(8, 2, SUB, WIDE)
            later = index + DEPTH

            @pl.when(later < 2 * CHUNKS)
            def _():
                next_g = later // CHUNKS
                for half in range(2):
                    input_copy(next_g, later - next_g * CHUNKS, half).start()

            @pl.when(jnp.logical_and(index == 1, g == 0))
            def _():
                pl.semaphore_wait(barrier, peers - 1)

            @pl.when(jnp.logical_and(lax.rem(chunk, 2) == 0, chunk > 0))
            def _():
                send_cols(raw_a, col_a, 0, g, chunk // 2 - 1)

            return sum_one, sum_two

        zero = jnp.zeros((SUB, WIDE), F32)
        sum_one, sum_two = lax.fori_loop(0, CHUNKS, body, (zero, zero))
        send_sums(0, g, message_of(sum_one, sum_two, sum_a[...]))
        send_cols(raw_a, col_a, 0, g, STEPS - 1)
        send_ends(raw_a, row_a, cor_a, 0, g)
        return carry

    lax.fori_loop(0, 2, load_group, 0)
    for copy in weight_copies():
        copy.wait()

    def bias_row(index):
        return bias_rest[index].astype(F32)

    def first_conv(g, carry):
        finish_exchange(raw_a, col_a, row_a, cor_a, 0, g)
        scale, shift = half_affine(0, g, cast_a[...], norm_first[...], WIDE)
        activation(raw_a, act_a, col_a, row_a, cor_a, 0, g, scale, shift, 2)
        convolve(act_a, WIDE, lambda: wf[...].reshape(3072, WIDE), bias_row(0), raw_t, col_t, row_t, cor_t, 1, g)
        return carry

    lax.fori_loop(0, 2, first_conv, 0)

    def layer(src, norm_at, weights, bias, dst, par, g, **more):
        finish_exchange(src, col_t, row_t, cor_t, par, g)
        scale, shift = half_affine(par, g, cast_t[...], norm_rest[norm_at], LANES)
        activation(src, act_t, col_t, row_t, cor_t, par, g, scale, shift, 4)
        if weights is not None:
            convolve(act_t, LANES, weights, bias, dst, col_t, row_t, cor_t, 1 - par, g, **more)

    def shortcut_conv(g, carry):
        def extra(first):
            return [raw_a[g, pl.ds(first, BLOCK), :, which].reshape(BLOCK * LANES, WIDE) for which in range(2)]

        def weights():
            return jnp.concatenate([wr[0].reshape(1536, WIDE), ws[...].reshape(512, WIDE)], axis=0)

        layer(raw_t, 0, weights, bias_row(1) + bias_row(6), raw_h, 1, g, extra=extra)
        return carry

    lax.fori_loop(0, 2, shortcut_conv, 0)

    def resnet(res, carry):
        base = 2 * res + 1

        def first_half(g, inner):
            layer(raw_h, base, lambda: wr[base].reshape(1536, WIDE), bias_row(base + 1), raw_t, 0, g)
            return inner

        def second_half(g, inner):
            layer(raw_t, base + 1, lambda: wr[base + 1].reshape(1536, WIDE), bias_row(base + 2), raw_h, 1, g, residual=raw_h)
            return inner

        lax.fori_loop(0, 2, first_half, 0)
        lax.fori_loop(0, 2, second_half, 0)
        return carry

    lax.fori_loop(0, 2, resnet, 0)

    def out_conv(g, carry):
        layer(raw_h, 5, None, None, None, 0, g)

        def body(step, inner):
            taps = jnp.concatenate(windows(act_t, step * BLOCK, LANES), axis=1)
            out = lax.dot_general(wo[...], taps, (((1,), (1,)), ((), ())), preferred_element_type=F32)
            image[g, step] = out[0:8]
            return inner

        lax.fori_loop(0, STEPS, body, 0)
        return carry

    lax.fori_loop(0, 2, out_conv, 0)


def solution(mesh):
    rows_n = mesh.shape["sy"]
    cols_n = mesh.shape["sx"]
    tile_spec = P("dp", "sy", "sx", None)
    replicated = P()
    dma = pltpu.SemaphoreType.DMA

    def local_decode(act_in, norm_first, w_first, w_short, norm_rest, w_rest, bias_rest, w_out, bias_out):
        vmem = pl.BlockSpec(memory_space=pltpu.VMEM)
        anywhere = pl.BlockSpec(memory_space=pl.ANY)
        tall = pl.pallas_call(
            functools.partial(kernel, rows_n, cols_n),
            out_shape=jax.ShapeDtypeStruct((2, STEPS, 8, BLOCK * LANES), F32),
            in_specs=[anywhere, vmem, anywhere, anywhere, vmem, anywhere, vmem, vmem],
            out_specs=vmem,
            scratch_shapes=[
                pltpu.VMEM((DEPTH, 2, 8, CHUNK, SUB, WIDE), BF16),
                pltpu.VMEM((2, SLAB, 8, 2, SUB, WIDE), BF16),
                pltpu.VMEM((2, SLAB, 8, 2, SUB, LANES), BF16),
                pltpu.VMEM((2, SLAB, 8, 2, SUB, LANES), BF16),
                pltpu.VMEM((SLAB + 2, 9, 2, SUB, WIDE), BF16),
                pltpu.VMEM((SLAB + 2, 9, 2, SUB, LANES), BF16),
                pltpu.VMEM((3, 4, WIDE, WIDE), BF16),
                pltpu.VMEM((2, WIDE, WIDE), BF16),
                pltpu.VMEM((5, 3, 4, LANES, WIDE), BF16),
                pltpu.VMEM((SUB, 1536), BF16),
                pltpu.VMEM((WIDE, WIDE), BF16),
                pltpu.VMEM((512, LANES), BF16),
                pltpu.VMEM((WIDE, LANES), BF16),
                pltpu.VMEM((LANES, 512), BF16),
                pltpu.VMEM((LANES, WIDE), BF16),
                pltpu.VMEM((1, 2, 2, SLAB, SUB, WIDE), BF16),
                pltpu.VMEM((1, 2, 2, 8, 2, SUB, WIDE), BF16),
                pltpu.VMEM((1, 2, 2, 2, SUB, WIDE), BF16),
                pltpu.VMEM((2, 2, 2, SLAB, SUB, LANES), BF16),
                pltpu.VMEM((2, 2, 2, 8, 2, SUB, LANES), BF16),
                pltpu.VMEM((2, 2, 2, 2, SUB, LANES), BF16),
                pltpu.VMEM((2, 2, rows_n * cols_n, 8, LANES), F32),
                dma((DEPTH, 2)),
                dma((3, 2)),
                dma((2, 2, 2)),
                dma((2, 2, 2)),
                dma((2, 2, 2)),
                dma((2, 2, 2)),
                dma((2, 2, 2, 2)),
                dma((2, 2, 2, 2)),
                dma((2, 2)),
                dma((2, 2)),
            ],
            compiler_params=pltpu.CompilerParams(collective_id=0, has_side_effects=True, vmem_limit_bytes=62 << 20),
            name="decode",
        )(act_in, norm_first, w_first, w_short, norm_rest, w_rest, bias_rest.reshape(7, 1, LANES), jnp.transpose(w_out, (0, 1, 3, 2)))
        parts = tall[:, :, :6].reshape(2, STEPS, 2, 3, BLOCK, 8, 2, 8)
        image = jnp.transpose(parts, (0, 7, 6, 1, 4, 5, 2, 3)).reshape(SUB, 2 * SLAB, SUB, 3)
        return image + bias_out.astype(F32)

    return jax.shard_map(local_decode, mesh=mesh, in_specs=(tile_spec, replicated, replicated, replicated, replicated, replicated, replicated, replicated, replicated), out_specs=tile_spec, check_vma=False)
```

```python
import functools

import jax
import jax.numpy as jnp
from jax import lax
from jax.experimental import pallas as pl
from jax.experimental.pallas import tpu as pltpu
from jax.sharding import PartitionSpec as P

GROUPS = 32
GN_EPS = 1e-6
MESH = pl.DeviceIdType.MESH
F32 = jnp.float32
LANES = 128
WIDE = 256
SUB = 16
BF16 = jnp.bfloat16
SLAB = 48
BLOCK = 16
STEPS = SLAB // BLOCK
CHUNK = 4
DEPTH = 3
CHUNKS = SLAB // CHUNK


def exact_rows(values):
    high = values.astype(BF16).astype(F32)
    rest = values - high
    mid = rest.astype(BF16).astype(F32)
    low = rest - mid
    return jnp.concatenate([high, mid, low, jnp.zeros_like(low)], axis=0).astype(BF16)


def exact_dot(values, ones):
    out = jnp.dot(exact_rows(values), ones, preferred_element_type=F32)
    return (out[0:8] + out[8:SUB]) + out[SUB:24]


def group_matrix(channels, transposed):
    per_group = channels // GROUPS
    shape = (LANES, 2 * channels) if transposed else (2 * channels, LANES)
    chan = lax.broadcasted_iota(jnp.int32, shape, 1 if transposed else 0)
    lane = lax.broadcasted_iota(jnp.int32, shape, 0 if transposed else 1)
    target = jnp.where(chan < channels, chan // per_group, GROUPS + (chan - channels) // per_group)
    return jnp.where(target == lane, 1.0, 0.0).astype(BF16)


def kernel(rows_n, cols_n, act_in, norm_first, w_first, w_short, norm_rest, w_rest, bias_rest, w_out, image,
           flat, order, bias_f, stage, raw_a, raw_t, raw_h, act_a, act_t, wf, ws, wr, wo, perm, sum_a, sum_t, cast_a, cast_t,
           col_a, row_a, cor_a, col_t, row_t, cor_t, slots,
           in_sem, wt_sem, col_send, col_recv, row_send, row_recv, cor_send, cor_recv, stat_send, stat_recv):
    peers = rows_n * cols_n
    my_x = lax.axis_index("sx")
    my_y = lax.axis_index("sy")
    me = my_x * rows_n + my_y
    has_side = (my_x > 0, my_x < cols_n - 1)
    has_end = (my_y > 0, my_y < rows_n - 1)
    count = float(rows_n * cols_n * 2 * SLAB * SUB)

    def at(dx, dy):
        return {"sx": my_x + dx, "sy": my_y + dy}

    def peer(index):
        return {"sx": index // rows_n, "sy": lax.rem(index, rows_n)}

    def col_copy(raw, col, par, g, side, start, size):
        src = raw.at[g, pl.ds(start, size), 0 if side == 0 else 7, side]
        dst = col.at[par, g, 1 - side, pl.ds(start, size)]
        return pltpu.make_async_remote_copy(src, dst, col_send.at[par, g, side], col_recv.at[par, g, 1 - side], device_id=at(2 * side - 1, 0), device_id_type=MESH)

    def row_copy(raw, row, par, g, end):
        src = raw.at[g, 0 if end == 0 else SLAB - 1]
        return pltpu.make_async_remote_copy(src, row.at[par, g, 1 - end], row_send.at[par, g, end], row_recv.at[par, g, 1 - end], device_id=at(0, 2 * end - 1), device_id_type=MESH)

    def cor_copy(raw, cor, par, g, end, side):
        src = raw.at[g, 0 if end == 0 else SLAB - 1, 0 if side == 0 else 7, side]
        return pltpu.make_async_remote_copy(src, cor.at[par, g, 1 - end, 1 - side], cor_send.at[par, g, end, side], cor_recv.at[par, g, 1 - end, 1 - side], device_id=at(2 * side - 1, 2 * end - 1), device_id_type=MESH)

    def stat_copy(par, g, offset):
        return pltpu.make_async_remote_copy(slots.at[par, g, me], slots.at[par, g, me], stat_send.at[par, g], stat_recv.at[par, g], device_id=peer(lax.rem(me + offset, peers)), device_id_type=MESH)

    def send_cols(raw, col, par, g, start, size):
        for side in range(2):
            @pl.when(has_side[side])
            def _():
                col_copy(raw, col, par, g, side, start, size).start()

    def send_ends(raw, row, cor, par, g):
        for end in range(2):
            @pl.when(has_end[end])
            def _():
                row_copy(raw, row, par, g, end).start()
            for side in range(2):
                @pl.when(jnp.logical_and(has_end[end], has_side[side]))
                def _():
                    cor_copy(raw, cor, par, g, end, side).start()

    def send_sums(par, g, message):
        slots[par, g, me] = message

        def one(offset, carry):
            stat_copy(par, g, offset).start()
            return carry

        lax.fori_loop(1, peers, one, 0)

    def finish_exchange(raw, col, row, cor, par, g):
        for side in range(2):
            @pl.when(has_side[side])
            def _():
                col_copy(raw, col, par, g, side, 0, SLAB).wait_send()
                col_copy(raw, col, par, g, 1 - side, 0, SLAB).wait_recv()
        for end in range(2):
            @pl.when(has_end[end])
            def _():
                row_copy(raw, row, par, g, end).wait_send()
                row_copy(raw, row, par, g, 1 - end).wait_recv()
            for side in range(2):
                @pl.when(jnp.logical_and(has_end[end], has_side[side]))
                def _():
                    cor_copy(raw, cor, par, g, end, side).wait_send()
                    cor_copy(raw, cor, par, g, 1 - end, 1 - side).wait_recv()
        arrived = slots.at[par, g, pl.ds(0, peers - 1)]
        done = pltpu.make_async_remote_copy(arrived, arrived, stat_send.at[par, g], stat_recv.at[par, g], device_id=peer(lax.rem(me + 1, peers)), device_id_type=MESH)
        done.wait_send()
        done.wait_recv()

    def message_of(sum_one, sum_two, ones):
        both = jnp.concatenate([sum_one[0:8] + sum_one[8:SUB], sum_two[0:8] + sum_two[8:SUB]], axis=1)
        return exact_dot(both, ones)

    def half_affine(par, g, spread, norm_pair, channels):
        totals = slots[par, g, 0]
        for index in range(1, peers):
            totals = totals + slots[par, g, index]
        sums = exact_dot(totals, spread)
        inv_count = 1.0 / (count * (channels // GROUPS))
        mean = sums[:, :channels] * inv_count
        inv_std = lax.rsqrt(sums[:, channels:] * inv_count - mean * mean + GN_EPS)
        pair = norm_pair.astype(F32)
        scale = inv_std * pair[0:1]
        shift = pair[1:2] - mean * scale
        scale, shift = scale * 0.5, shift * 0.5
        return jnp.concatenate([scale, scale], axis=0), jnp.concatenate([shift, shift], axis=0)

    def activate(values, scale, shift):
        half = values.astype(F32) * scale + shift
        return half + half * jnp.tanh(half)

    def activation(raw, act, col, row, cor, par, g, scale, shift, block):
        def body(step, carry):
            first = step * block
            out = activate(raw[g, pl.ds(first, block)], scale, shift).astype(BF16)
            act[pl.ds(first + 1, block), 0:8, 1] = out[:, :, 0]
            act[pl.ds(first + 1, block), 1:9, 0] = out[:, :, 1]
            for side in range(2):
                edge = activate(col[par, g, side, pl.ds(first, block)], scale, shift)
                act[pl.ds(first + 1, block), 8 * side, side] = jnp.where(has_side[side], edge, 0.0).astype(BF16)
            return carry

        lax.fori_loop(0, SLAB // block, body, 0)
        for end in range(2):
            keep, other = (slice(8, SUB), slice(0, 8)) if end == 0 else (slice(0, 8), slice(8, SUB))
            dest = 0 if end == 0 else SLAB + 1
            inner = SLAB if end == 0 else 1

            def put(pair_at, which, remote, present):
                mine = act[inner, pair_at, which].astype(F32)
                far = jnp.where(present, remote, 0.0)[..., keep, :]
                near = mine[..., other, :]
                parts = [far, near] if end == 0 else [near, far]
                act[dest, pair_at, which] = jnp.concatenate(parts, axis=-2).astype(BF16)

            line = activate(row[par, g, end], scale, shift)
            put(slice(0, 8), 1, line[:, 0], has_end[end])
            put(slice(1, 9), 0, line[:, 1], has_end[end])
            for side in range(2):
                spot = activate(cor[par, g, end, side], scale, shift)
                put(8 * side, side, spot, jnp.logical_and(has_end[end], has_side[side]))

    def windows(act, first, channels):
        taps = []
        for row_off in range(3):
            for col_off in range(4):
                pair_at = col_off // 2
                taps.append(act[pl.ds(first + row_off, BLOCK), pair_at:pair_at + 8, col_off % 2].reshape(BLOCK * LANES, channels))
        return taps

    def convolve(act, channels, weights, bias, dst, col, row, cor, par, g, extra=None, residual=None):
        bias_pair = jnp.concatenate([bias, bias], axis=1)

        def body(step, carry):
            sum_one, sum_two = carry
            first = step * BLOCK
            taps = windows(act, first, channels)
            if extra is not None:
                taps = taps + extra(first)
            out = jnp.dot(jnp.concatenate(taps, axis=1), weights(), preferred_element_type=F32) + bias_pair
            if residual is not None:
                kept = residual[g, pl.ds(first, BLOCK)].astype(F32)
                kept = jnp.concatenate([kept[:, :, 0], kept[:, :, 1]], axis=-1)
                out = out + kept.reshape(BLOCK * LANES, WIDE)
            rounded = out.astype(BF16)
            wide = rounded.astype(F32).reshape(BLOCK * 8, SUB, WIDE)
            sum_one = sum_one + jnp.sum(wide, axis=0)
            sum_two = sum_two + jnp.sum(wide * wide, axis=0)
            tiles = rounded.reshape(BLOCK, 8, SUB, WIDE)
            dst[g, pl.ds(first, BLOCK), :, 0] = tiles[..., :LANES]
            dst[g, pl.ds(first, BLOCK), :, 1] = tiles[..., LANES:]

            @pl.when(step > 0)
            def _():
                send_cols(dst, col, par, g, (step - 1) * BLOCK, BLOCK)

            return sum_one, sum_two

        zero = jnp.zeros((SUB, WIDE), F32)
        sum_one, sum_two = lax.fori_loop(0, STEPS, body, (zero, zero))
        send_sums(par, g, message_of(sum_one[:, :LANES] + sum_one[:, LANES:], sum_two[:, :LANES] + sum_two[:, LANES:], sum_t[...]))
        send_cols(dst, col, par, g, SLAB - BLOCK, BLOCK)
        send_ends(dst, row, cor, par, g)

    def input_copy(g, chunk, half):
        index = g * CHUNKS + chunk
        slot = lax.rem(index, DEPTH)
        src = act_in.at[pl.ds(g * 8, 8), pl.ds(half * SLAB + chunk * CHUNK, CHUNK)]
        return pltpu.make_async_copy(src, stage.at[slot, half], in_sem.at[slot, half])

    for early in range(DEPTH):
        for half in range(2):
            input_copy(0, early, half).start()

    barrier = pltpu.get_barrier_semaphore()

    def greet(offset, carry):
        pl.semaphore_signal(barrier, inc=1, device_id=peer(lax.rem(me + offset, peers)), device_id_type=MESH)
        return carry

    lax.fori_loop(1, peers, greet, 0)

    out_row = lax.broadcasted_iota(jnp.int32, (WIDE, WIDE), 0)
    in_row = lax.broadcasted_iota(jnp.int32, (WIDE, WIDE), 1)
    swapped = jnp.logical_and(out_row // SUB == in_row % SUB, out_row % SUB == in_row // SUB)
    perm[...] = jnp.where(swapped, 1.0, 0.0).astype(BF16)
    shape = (LANES, 2 * WIDE)
    target = lax.broadcasted_iota(jnp.int32, shape, 0)
    lane = lax.broadcasted_iota(jnp.int32, shape, 1)
    half_at, col_at, pair_at = lane // WIDE, lane // LANES % 2, lane // SUB % 8
    wanted = jnp.logical_and(lane // 8 % 2 == half_at, target == lane % 8 * SUB + 2 * pair_at + col_at)
    order[...] = jnp.where(wanted, 1.0, 0.0).astype(BF16)
    bias_f[0:7] = bias_rest[...].astype(F32)
    sum_a[...] = group_matrix(WIDE, False)
    sum_t[...] = group_matrix(LANES, False)
    cast_a[...] = group_matrix(WIDE, True)
    cast_t[...] = group_matrix(LANES, True)
    for tap in range(3):
        wf[tap, 3, :, 0:LANES] = jnp.zeros((WIDE, LANES), BF16)
        wf[tap, 0, :, LANES:WIDE] = jnp.zeros((WIDE, LANES), BF16)
        for layer in range(5):
            wr[layer, tap, 3, :, 0:LANES] = jnp.zeros((LANES, LANES), BF16)
            wr[layer, tap, 0, :, LANES:WIDE] = jnp.zeros((LANES, LANES), BF16)
    ws[0, :, LANES:WIDE] = jnp.zeros((WIDE, LANES), BF16)
    ws[1, :, 0:LANES] = jnp.zeros((WIDE, LANES), BF16)

    def weight_copies():
        copies = []
        for out_col in range(2):
            lanes = pl.ds(out_col * LANES, LANES)
            copies.append(pltpu.make_async_copy(w_first, wf.at[:, pl.ds(out_col, 3), :, lanes], wt_sem.at[0, out_col]))
            copies.append(pltpu.make_async_copy(w_short, ws.at[out_col, :, lanes], wt_sem.at[1, out_col]))
            copies.append(pltpu.make_async_copy(w_rest, wr.at[:, :, pl.ds(out_col, 3), :, lanes], wt_sem.at[2, out_col]))
        return copies

    for copy in weight_copies():
        copy.start()

    blank = jnp.zeros((3, LANES), F32)
    for row_off in range(3):
        for col_off in range(4):
            parts = []
            for out_col in range(2):
                tap = col_off - out_col
                parts.append(w_out[row_off, tap].astype(F32) if 0 <= tap < 3 else blank)
            parts.append(jnp.zeros((10, LANES), F32))
            at_lane = (row_off * 4 + col_off) * LANES
            wo[:, at_lane:at_lane + LANES] = jnp.concatenate(parts, axis=0).astype(BF16)

    def load_group(g, carry):
        def body(chunk, sums):
            sum_one, sum_two = sums
            index = g * CHUNKS + chunk
            slot = lax.rem(index, DEPTH)
            for half in range(2):
                input_copy(g, chunk, half).wait()
            for line in range(CHUNK):
                tile = stage[slot, :, :, line].reshape(WIDE, WIDE)
                out = jnp.dot(perm[...], tile, preferred_element_type=F32)
                cube = out.reshape(SUB, SUB, WIDE)
                sum_one = sum_one + jnp.sum(cube, axis=0)
                sum_two = sum_two + jnp.sum(cube * cube, axis=0)
                raw_a[g, chunk * CHUNK + line] = out.astype(BF16).reshape(8, 2, SUB, WIDE)
            later = index + DEPTH

            @pl.when(later < 2 * CHUNKS)
            def _():
                next_g = later // CHUNKS
                for half in range(2):
                    input_copy(next_g, later - next_g * CHUNKS, half).start()

            @pl.when(index == 1)
            def _():
                pl.semaphore_wait(barrier, peers - 1)

            @pl.when(chunk > 0)
            def _():
                send_cols(raw_a, col_a, 0, g, (chunk - 1) * CHUNK, CHUNK)

            return sum_one, sum_two

        zero = jnp.zeros((SUB, WIDE), F32)
        sum_one, sum_two = lax.fori_loop(0, CHUNKS, body, (zero, zero))
        send_sums(0, g, message_of(sum_one, sum_two, sum_a[...]))
        send_cols(raw_a, col_a, 0, g, SLAB - CHUNK, CHUNK)
        send_ends(raw_a, row_a, cor_a, 0, g)
        return carry

    lax.fori_loop(0, 2, load_group, 0)
    for copy in weight_copies():
        copy.wait()

    def bias_row(index):
        return bias_f[pl.ds(index, 1)]

    def first_conv(g, carry):
        finish_exchange(raw_a, col_a, row_a, cor_a, 0, g)
        scale, shift = half_affine(0, g, cast_a[...], norm_first[...], WIDE)
        activation(raw_a, act_a, col_a, row_a, cor_a, 0, g, scale, shift, 2)
        convolve(act_a, WIDE, lambda: wf[...].reshape(3072, WIDE), bias_row(0), raw_t, col_t, row_t, cor_t, 1, g)
        return carry

    lax.fori_loop(0, 2, first_conv, 0)

    def layer(src, norm_at, weights, bias, dst, par, g, **more):
        finish_exchange(src, col_t, row_t, cor_t, par, g)
        scale, shift = half_affine(par, g, cast_t[...], norm_rest[norm_at], LANES)
        activation(src, act_t, col_t, row_t, cor_t, par, g, scale, shift, 4)
        if weights is not None:
            convolve(act_t, LANES, weights, bias, dst, col_t, row_t, cor_t, 1 - par, g, **more)

    def shortcut_conv(g, carry):
        def extra(first):
            return [raw_a[g, pl.ds(first, BLOCK), :, which].reshape(BLOCK * LANES, WIDE) for which in range(2)]

        def weights():
            return jnp.concatenate([wr[0].reshape(1536, WIDE), ws[...].reshape(512, WIDE)], axis=0)

        layer(raw_t, 0, weights, bias_row(1) + bias_row(6), raw_h, 1, g, extra=extra)
        return carry

    lax.fori_loop(0, 2, shortcut_conv, 0)

    def resnet(res, carry):
        base = 2 * res + 1

        def first_half(g, inner):
            layer(raw_h, base, lambda: wr[base].reshape(1536, WIDE), bias_row(base + 1), raw_t, 0, g)
            return inner

        def second_half(g, inner):
            layer(raw_t, base + 1, lambda: wr[base + 1].reshape(1536, WIDE), bias_row(base + 2), raw_h, 1, g, residual=raw_h)
            return inner

        lax.fori_loop(0, 2, first_half, 0)
        lax.fori_loop(0, 2, second_half, 0)
        return carry

    lax.fori_loop(0, 2, resnet, 0)

    def out_conv(g, carry):
        layer(raw_h, 5, None, None, None, 0, g)

        def body(step, inner):
            taps = jnp.concatenate(windows(act_t, step * BLOCK, LANES), axis=1)
            out = lax.dot_general(wo[...], taps, (((1,), (1,)), ((), ())), preferred_element_type=F32)
            for line in range(BLOCK):
                flat[pl.ds(step * BLOCK + line, 8, stride=SLAB), :] = out[0:8, line * LANES:(line + 1) * LANES]
            return inner

        lax.fori_loop(0, STEPS, body, 0)
        for channel in range(3):
            lines = [flat[pl.ds((3 * out_col + channel) * SLAB, SLAB), :] for out_col in range(2)]
            values = jnp.concatenate(lines, axis=1)
            total = jnp.zeros((LANES, 2 * SLAB), F32)
            for _ in range(3):
                term = values.astype(BF16)
                values = values - term.astype(F32)
                blank_half = jnp.zeros_like(term)
                spread = jnp.concatenate([jnp.concatenate([term, blank_half], axis=1), jnp.concatenate([blank_half, term], axis=1)], axis=0)
                total = total + lax.dot_general(order[...], spread, (((1,), (1,)), ((), ())), preferred_element_type=F32)
            image[pl.ds(g * 8, 8), channel] = total.reshape(8, SUB, 2 * SLAB)
        return carry

    lax.fori_loop(0, 2, out_conv, 0)


def solution(mesh):
    rows_n = mesh.shape["sy"]
    cols_n = mesh.shape["sx"]
    tile_spec = P("dp", "sy", "sx", None)
    replicated = P()
    dma = pltpu.SemaphoreType.DMA

    def local_decode(act_in, norm_first, w_first, w_short, norm_rest, w_rest, bias_rest, w_out, bias_out):
        vmem = pl.BlockSpec(memory_space=pltpu.VMEM)
        anywhere = pl.BlockSpec(memory_space=pl.ANY)
        planes = pl.pallas_call(
            functools.partial(kernel, rows_n, cols_n),
            out_shape=jax.ShapeDtypeStruct((SUB, 3, SUB, 2 * SLAB), F32),
            in_specs=[anywhere, vmem, anywhere, anywhere, vmem, anywhere, vmem, vmem],
            out_specs=vmem,
            scratch_shapes=[
                pltpu.VMEM((8 * SLAB, LANES), F32),
                pltpu.VMEM((LANES, 2 * WIDE), BF16),
                pltpu.VMEM((8, LANES), F32),
                pltpu.VMEM((DEPTH, 2, 8, CHUNK, SUB, WIDE), BF16),
                pltpu.VMEM((2, SLAB, 8, 2, SUB, WIDE), BF16),
                pltpu.VMEM((2, SLAB, 8, 2, SUB, LANES), BF16),
                pltpu.VMEM((2, SLAB, 8, 2, SUB, LANES), BF16),
                pltpu.VMEM((SLAB + 2, 9, 2, SUB, WIDE), BF16),
                pltpu.VMEM((SLAB + 2, 9, 2, SUB, LANES), BF16),
                pltpu.VMEM((3, 4, WIDE, WIDE), BF16),
                pltpu.VMEM((2, WIDE, WIDE), BF16),
                pltpu.VMEM((5, 3, 4, LANES, WIDE), BF16),
                pltpu.VMEM((SUB, 1536), BF16),
                pltpu.VMEM((WIDE, WIDE), BF16),
                pltpu.VMEM((512, LANES), BF16),
                pltpu.VMEM((WIDE, LANES), BF16),
                pltpu.VMEM((LANES, 512), BF16),
                pltpu.VMEM((LANES, WIDE), BF16),
                pltpu.VMEM((1, 2, 2, SLAB, SUB, WIDE), BF16),
                pltpu.VMEM((1, 2, 2, 8, 2, SUB, WIDE), BF16),
                pltpu.VMEM((1, 2, 2, 2, SUB, WIDE), BF16),
                pltpu.VMEM((2, 2, 2, SLAB, SUB, LANES), BF16),
                pltpu.VMEM((2, 2, 2, 8, 2, SUB, LANES), BF16),
                pltpu.VMEM((2, 2, 2, 2, SUB, LANES), BF16),
                pltpu.VMEM((2, 2, rows_n * cols_n, 8, LANES), F32),
                dma((DEPTH, 2)),
                dma((3, 2)),
                dma((2, 2, 2)),
                dma((2, 2, 2)),
                dma((2, 2, 2)),
                dma((2, 2, 2)),
                dma((2, 2, 2, 2)),
                dma((2, 2, 2, 2)),
                dma((2, 2)),
                dma((2, 2)),
            ],
            compiler_params=pltpu.CompilerParams(collective_id=0, has_side_effects=True, vmem_limit_bytes=62 << 20),
            name="decode",
        )(act_in, norm_first, w_first, w_short, norm_rest, w_rest, bias_rest, jnp.transpose(w_out, (0, 1, 3, 2)))
        return jnp.transpose(planes, (0, 3, 2, 1)) + bias_out.astype(F32)

    return jax.shard_map(local_decode, mesh=mesh, in_specs=(tile_spec, replicated, replicated, replicated, replicated, replicated, replicated, replicated, replicated), out_specs=tile_spec, check_vma=False)
```

```python
import functools

import jax
import jax.numpy as jnp
from jax import lax
from jax.experimental import pallas as pl
from jax.experimental.pallas import tpu as pltpu
from jax.sharding import PartitionSpec as P

GROUPS = 32
GN_EPS = 1e-6
MESH = pl.DeviceIdType.MESH
F32 = jnp.float32
LANES = 128
WIDE = 256
SUB = 16
BF16 = jnp.bfloat16
SLAB = 48
BLOCK = 8
STEPS = SLAB // BLOCK
EARLY = 4
CHUNK = 4
DEPTH = 8
CHUNKS = SLAB // CHUNK


def exact_rows(values):
    high = values.astype(BF16).astype(F32)
    rest = values - high
    mid = rest.astype(BF16).astype(F32)
    low = rest - mid
    return jnp.concatenate([high, mid, low, jnp.zeros_like(low)], axis=0).astype(BF16)


def exact_dot(values, ones):
    out = jnp.dot(exact_rows(values), ones, preferred_element_type=F32)
    return (out[0:8] + out[8:SUB]) + out[SUB:24]


def group_matrix(channels, transposed):
    per_group = channels // GROUPS
    shape = (LANES, 2 * channels) if transposed else (2 * channels, LANES)
    chan = lax.broadcasted_iota(jnp.int32, shape, 1 if transposed else 0)
    lane = lax.broadcasted_iota(jnp.int32, shape, 0 if transposed else 1)
    target = jnp.where(chan < channels, chan // per_group, GROUPS + (chan - channels) // per_group)
    return jnp.where(target == lane, 1.0, 0.0).astype(BF16)


def kernel(rows_n, cols_n, act_in, norm_first, w_first, w_short, norm_rest, w_rest, bias_rest, w_out, image,
           flat, order, bias_f, stage, raw_a, raw_t, raw_h, act_a0, act_a1, act_a2, act_t0, act_t1, act_t2, wf, ws, wr, wo, perm, sum_a, sum_t, cast_a, cast_t,
           col_a, row_a, cor_a, col_t, row_t, cor_t, slots,
           in_sem, wt_sem, col_send, col_recv, row_send, row_recv, cor_send, cor_recv, stat_send, stat_recv):
    peers = rows_n * cols_n
    act_a = (act_a0, act_a1, act_a2)
    act_t = (act_t0, act_t1, act_t2)
    my_x = lax.axis_index("sx")
    my_y = lax.axis_index("sy")
    me = my_x * rows_n + my_y
    has_side = (my_x > 0, my_x < cols_n - 1)
    has_end = (my_y > 0, my_y < rows_n - 1)
    count = float(rows_n * cols_n * 2 * SLAB * SUB)

    def at(dx, dy):
        return {"sx": my_x + dx, "sy": my_y + dy}

    def peer(index):
        return {"sx": index // rows_n, "sy": lax.rem(index, rows_n)}

    def col_copy(raw, col, par, g, side, start, size):
        src = raw.at[g, pl.ds(start, size), 0 if side == 0 else 7, side]
        dst = col.at[par, g, 1 - side, pl.ds(start, size)]
        return pltpu.make_async_remote_copy(src, dst, col_send.at[par, g, side], col_recv.at[par, g, 1 - side], device_id=at(2 * side - 1, 0), device_id_type=MESH)

    def row_copy(raw, row, par, g, end):
        src = raw.at[g, 0 if end == 0 else SLAB - 1]
        return pltpu.make_async_remote_copy(src, row.at[par, g, 1 - end], row_send.at[par, g, end], row_recv.at[par, g, 1 - end], device_id=at(0, 2 * end - 1), device_id_type=MESH)

    def cor_copy(raw, cor, par, g, end, side):
        src = raw.at[g, 0 if end == 0 else SLAB - 1, 0 if side == 0 else 7, side]
        return pltpu.make_async_remote_copy(src, cor.at[par, g, 1 - end, 1 - side], cor_send.at[par, g, end, side], cor_recv.at[par, g, 1 - end, 1 - side], device_id=at(2 * side - 1, 2 * end - 1), device_id_type=MESH)

    def stat_copy(par, g, offset):
        return pltpu.make_async_remote_copy(slots.at[par, g, me], slots.at[par, g, me], stat_send.at[par, g], stat_recv.at[par, g], device_id=peer(lax.rem(me + offset, peers)), device_id_type=MESH)

    def send_cols(raw, col, par, g, start, size):
        for side in range(2):
            @pl.when(has_side[side])
            def _():
                col_copy(raw, col, par, g, side, start, size).start()

    def send_ends(raw, row, cor, par, g):
        for end in range(2):
            @pl.when(has_end[end])
            def _():
                row_copy(raw, row, par, g, end).start()
            for side in range(2):
                @pl.when(jnp.logical_and(has_end[end], has_side[side]))
                def _():
                    cor_copy(raw, cor, par, g, end, side).start()

    def send_sums(par, g, message):
        slots[par, g, me] = message

        def one(offset, carry):
            stat_copy(par, g, offset).start()
            return carry

        lax.fori_loop(1, peers, one, 0)

    def finish_exchange(raw, col, row, cor, par, g):
        for side in range(2):
            @pl.when(has_side[side])
            def _():
                col_copy(raw, col, par, g, side, 0, SLAB).wait_send()
                col_copy(raw, col, par, g, 1 - side, 0, SLAB).wait_recv()
        for end in range(2):
            @pl.when(has_end[end])
            def _():
                row_copy(raw, row, par, g, end).wait_send()
                row_copy(raw, row, par, g, 1 - end).wait_recv()
            for side in range(2):
                @pl.when(jnp.logical_and(has_end[end], has_side[side]))
                def _():
                    cor_copy(raw, cor, par, g, end, side).wait_send()
                    cor_copy(raw, cor, par, g, 1 - end, 1 - side).wait_recv()
        arrived = slots.at[par, g, pl.ds(0, peers - 1)]
        done = pltpu.make_async_remote_copy(arrived, arrived, stat_send.at[par, g], stat_recv.at[par, g], device_id=peer(lax.rem(me + 1, peers)), device_id_type=MESH)
        done.wait_send()
        done.wait_recv()

    def message_of(sum_one, sum_two, ones):
        both = jnp.concatenate([sum_one[0:8] + sum_one[8:SUB], sum_two[0:8] + sum_two[8:SUB]], axis=1)
        return exact_dot(both, ones)

    def half_affine(par, g, spread, norm_pair, channels):
        totals = slots[par, g, 0]
        for index in range(1, peers):
            totals = totals + slots[par, g, index]
        sums = exact_dot(totals, spread)
        inv_count = 1.0 / (count * (channels // GROUPS))
        mean = sums[:, :channels] * inv_count
        inv_std = lax.rsqrt(sums[:, channels:] * inv_count - mean * mean + GN_EPS)
        pair = norm_pair.astype(F32)
        scale = inv_std * pair[0:1]
        shift = pair[1:2] - mean * scale
        scale, shift = scale * 0.5, shift * 0.5
        return jnp.concatenate([scale, scale], axis=0), jnp.concatenate([shift, shift], axis=0)

    def activate(values, scale, shift):
        half = values.astype(F32) * scale + shift
        return half + half * jnp.tanh(half)

    def activation(raw, act, col, row, cor, par, g, scale, shift):
        def rows(ring, local, first, size):
            out = activate(raw[g, first:first + size], scale, shift).astype(BF16)
            ring[local:local + size, 0:8, 1] = out[:, :, 0]
            ring[local:local + size, 1:9, 0] = out[:, :, 1]
            for side in range(2):
                edge = activate(col[par, g, side, first:first + size], scale, shift)
                ring[local:local + size, 8 * side, side] = jnp.where(has_side[side], edge, 0.0).astype(BF16)

        def outer_row(ring, local, end):
            inner = SLAB - 1 if end == 0 else 0
            low, high = slice(0, 8), slice(8, SUB)
            own, far = (low, high) if end == 0 else (high, low)

            def join(mine, theirs, mine_present, theirs_present):
                near = activate(mine.astype(F32)[..., own, :], scale[0:8], shift[0:8])
                away = activate(theirs.astype(F32)[..., far, :], scale[0:8], shift[0:8])
                if mine_present is not None:
                    near = jnp.where(mine_present, near, 0.0)
                away = jnp.where(theirs_present, away, 0.0)
                return jnp.concatenate([away, near] if end == 0 else [near, away], axis=-2).astype(BF16)

            line = join(raw[g, inner], row[par, g, end], None, has_end[end])
            ring[local, 0:8, 1] = line[:, 0]
            ring[local, 1:9, 0] = line[:, 1]
            for side in range(2):
                both = jnp.logical_and(has_end[end], has_side[side])
                ring[local, 8 * side, side] = join(col[par, g, side, inner], cor[par, g, end, side], has_side[side], both)

        def chunk(index):
            ring = act[index % 3]
            if index < 0:
                outer_row(ring, BLOCK - 2, 0)
                rows(ring, BLOCK - 1, 0, 1)
            elif index < STEPS - 1:
                rows(ring, 0, index * BLOCK + 1, BLOCK)
            elif index == STEPS - 1:
                rows(ring, 0, index * BLOCK + 1, BLOCK - 1)
                outer_row(ring, BLOCK - 1, 1)

        return chunk

    def window(act, index, row_off, col_off, channels):
        pair_at = slice(col_off // 2, col_off // 2 + 8)
        which = col_off % 2
        low = row_off - 2
        if low == 0:
            out = act[index % 3][:, pair_at, which]
        else:
            out = jnp.concatenate([act[(index - 1) % 3][BLOCK + low:BLOCK, pair_at, which], act[index % 3][0:BLOCK + low, pair_at, which]], axis=0)
        return out.reshape(BLOCK * LANES, channels)

    def convolve(act, chunk, channels, weights, bias, dst, col, row, cor, par, g, extra=None, residual=None):
        bias_pair = jnp.concatenate([bias, bias], axis=1)
        sum_one = sum_two = jnp.zeros((SUB, WIDE), F32)
        chunk(-1)
        chunk(0)
        for step in range(STEPS):
            span = slice(step * BLOCK, step * BLOCK + BLOCK)
            taps = [window(act, step, row_off, col_off, channels) for row_off in range(3) for col_off in range(4)]
            if extra is not None:
                taps = taps + extra(span)
            out = jnp.dot(jnp.concatenate(taps, axis=1), weights(), preferred_element_type=F32) + bias_pair
            if residual is not None:
                kept = residual[g, span].astype(F32)
                kept = jnp.concatenate([kept[:, :, 0], kept[:, :, 1]], axis=-1)
                out = out + kept.reshape(BLOCK * LANES, WIDE)
            rounded = out.astype(BF16)
            wide = rounded.astype(F32).reshape(BLOCK * 8, SUB, WIDE)
            sum_one = sum_one + jnp.sum(wide, axis=0)
            sum_two = sum_two + jnp.sum(wide * wide, axis=0)
            tiles = rounded.reshape(BLOCK, 8, SUB, WIDE)
            dst[g, span, :, 0] = tiles[..., :LANES]
            dst[g, span, :, 1] = tiles[..., LANES:]
            chunk(step + 1)
            if step == EARLY - 1:
                send_cols(dst, col, par, g, 0, EARLY * BLOCK)
        send_sums(par, g, message_of(sum_one[:, :LANES] + sum_one[:, LANES:], sum_two[:, :LANES] + sum_two[:, LANES:], sum_t[...]))
        send_ends(dst, row, cor, par, g)
        send_cols(dst, col, par, g, EARLY * BLOCK, SLAB - EARLY * BLOCK)

    def input_copy(g, chunk, half):
        index = g * CHUNKS + chunk
        slot = lax.rem(index, DEPTH)
        src = act_in.at[pl.ds(g * 8, 8), pl.ds(half * SLAB + chunk * CHUNK, CHUNK)]
        return pltpu.make_async_copy(src, stage.at[slot, half], in_sem.at[slot, half])

    for early in range(DEPTH):
        for half in range(2):
            input_copy(0, early, half).start()

    barrier = pltpu.get_barrier_semaphore()

    def greet(offset, carry):
        pl.semaphore_signal(barrier, inc=1, device_id=peer(lax.rem(me + offset, peers)), device_id_type=MESH)
        return carry

    lax.fori_loop(1, peers, greet, 0)

    out_row = lax.broadcasted_iota(jnp.int32, (WIDE, WIDE), 0)
    in_row = lax.broadcasted_iota(jnp.int32, (WIDE, WIDE), 1)
    swapped = jnp.logical_and(out_row // SUB == in_row % SUB, out_row % SUB == in_row // SUB)
    perm[...] = jnp.where(swapped, 1.0, 0.0).astype(BF16)
    shape = (LANES, 2 * WIDE)
    target = lax.broadcasted_iota(jnp.int32, shape, 0)
    lane = lax.broadcasted_iota(jnp.int32, shape, 1)
    half_at, col_at, pair_at = lane // WIDE, lane // LANES % 2, lane // SUB % 8
    wanted = jnp.logical_and(lane // 8 % 2 == half_at, target == lane % 8 * SUB + 2 * pair_at + col_at)
    order[...] = jnp.where(wanted, 1.0, 0.0).astype(BF16)
    bias_f[0:7] = bias_rest[...].astype(F32)
    sum_a[...] = group_matrix(WIDE, False)
    sum_t[...] = group_matrix(LANES, False)
    cast_a[...] = group_matrix(WIDE, True)
    cast_t[...] = group_matrix(LANES, True)
    for tap in range(3):
        wf[tap, 3, :, 0:LANES] = jnp.zeros((WIDE, LANES), BF16)
        wf[tap, 0, :, LANES:WIDE] = jnp.zeros((WIDE, LANES), BF16)
        for layer in range(5):
            wr[layer, tap, 3, :, 0:LANES] = jnp.zeros((LANES, LANES), BF16)
            wr[layer, tap, 0, :, LANES:WIDE] = jnp.zeros((LANES, LANES), BF16)
    ws[0, :, LANES:WIDE] = jnp.zeros((WIDE, LANES), BF16)
    ws[1, :, 0:LANES] = jnp.zeros((WIDE, LANES), BF16)

    def weight_copies(first):
        copies = []
        for out_col in range(2):
            lanes = pl.ds(out_col * LANES, LANES)
            if first:
                copies.append(pltpu.make_async_copy(w_first, wf.at[:, pl.ds(out_col, 3), :, lanes], wt_sem.at[0, out_col]))
            else:
                copies.append(pltpu.make_async_copy(w_short, ws.at[out_col, :, lanes], wt_sem.at[1, out_col]))
                copies.append(pltpu.make_async_copy(w_rest, wr.at[:, :, pl.ds(out_col, 3), :, lanes], wt_sem.at[2, out_col]))
        return copies

    for copy in weight_copies(True):
        copy.start()

    blank = jnp.zeros((3, LANES), F32)
    blocks = []
    for row_off in range(3):
        parts = []
        for col_off in range(4):
            taps = [w_out[row_off, col_off - out_col].astype(F32) if 0 <= col_off - out_col < 3 else blank for out_col in range(2)]
            parts.append(jnp.concatenate(taps + [blank[0:2]], axis=0))
        blocks.append(jnp.concatenate(parts, axis=1))
    blocks.append(jnp.zeros_like(blocks[0]))
    wo[...] = jnp.concatenate(blocks, axis=0).astype(BF16)

    def load_group(g, carry):
        def body(chunk, sums):
            sum_one, sum_two = sums
            index = g * CHUNKS + chunk
            slot = lax.rem(index, DEPTH)
            for half in range(2):
                input_copy(g, chunk, half).wait()
            for line in range(CHUNK):
                tile = stage[slot, :, :, line].reshape(WIDE, WIDE)
                out = jnp.dot(perm[...], tile, preferred_element_type=F32)
                cube = out.reshape(SUB, SUB, WIDE)
                sum_one = sum_one + jnp.sum(cube, axis=0)
                sum_two = sum_two + jnp.sum(cube * cube, axis=0)
                raw_a[g, chunk * CHUNK + line] = out.astype(BF16).reshape(8, 2, SUB, WIDE)
            later = index + DEPTH

            @pl.when(later < 2 * CHUNKS)
            def _():
                next_g = later // CHUNKS
                for half in range(2):
                    input_copy(next_g, later - next_g * CHUNKS, half).start()

            @pl.when(index == 1)
            def _():
                pl.semaphore_wait(barrier, peers - 1)

            @pl.when(chunk > 0)
            def _():
                send_cols(raw_a, col_a, 0, g, (chunk - 1) * CHUNK, CHUNK)

            return sum_one, sum_two

        zero = jnp.zeros((SUB, WIDE), F32)
        sum_one, sum_two = lax.fori_loop(0, CHUNKS, body, (zero, zero))
        send_sums(0, g, message_of(sum_one, sum_two, sum_a[...]))
        send_cols(raw_a, col_a, 0, g, SLAB - CHUNK, CHUNK)
        send_ends(raw_a, row_a, cor_a, 0, g)
        return carry

    lax.fori_loop(0, 2, load_group, 0)
    for copy in weight_copies(False):
        copy.start()
    for copy in weight_copies(True):
        copy.wait()

    def bias_row(index):
        return bias_f[pl.ds(index, 1)]

    def first_conv(g, carry):
        finish_exchange(raw_a, col_a, row_a, cor_a, 0, g)
        scale, shift = half_affine(0, g, cast_a[...], norm_first[...], WIDE)
        chunk = activation(raw_a, act_a, col_a, row_a, cor_a, 0, g, scale, shift)
        convolve(act_a, chunk, WIDE, lambda: wf[...].reshape(3072, WIDE), bias_row(0), raw_t, col_t, row_t, cor_t, 1, g)
        return carry

    lax.fori_loop(0, 2, first_conv, 0)
    for copy in weight_copies(False):
        copy.wait()

    def layer(src, norm_at, weights, bias, dst, par, g, **more):
        finish_exchange(src, col_t, row_t, cor_t, par, g)
        scale, shift = half_affine(par, g, cast_t[...], norm_rest[norm_at], LANES)
        chunk = activation(src, act_t, col_t, row_t, cor_t, par, g, scale, shift)
        if weights is not None:
            convolve(act_t, chunk, LANES, weights, bias, dst, col_t, row_t, cor_t, 1 - par, g, **more)
        return chunk

    def shortcut_conv(g, carry):
        def extra(span):
            return [raw_a[g, span, :, which].reshape(BLOCK * LANES, WIDE) for which in range(2)]

        def weights():
            return jnp.concatenate([wr[0].reshape(1536, WIDE), ws[...].reshape(512, WIDE)], axis=0)

        layer(raw_t, 0, weights, bias_row(1) + bias_row(6), raw_h, 1, g, extra=extra)
        return carry

    lax.fori_loop(0, 2, shortcut_conv, 0)

    def resnet(res, carry):
        base = 2 * res + 1

        def first_half(g, inner):
            layer(raw_h, base, lambda: wr[base].reshape(1536, WIDE), bias_row(base + 1), raw_t, 0, g)
            return inner

        def second_half(g, inner):
            layer(raw_t, base + 1, lambda: wr[base + 1].reshape(1536, WIDE), bias_row(base + 2), raw_h, 1, g, residual=raw_h)
            return inner

        lax.fori_loop(0, 2, first_half, 0)
        lax.fori_loop(0, 2, second_half, 0)
        return carry

    lax.fori_loop(0, 2, resnet, 0)

    def out_conv(g, carry):
        chunk = layer(raw_h, 5, None, None, None, 0, g)
        sums = {}

        def products(ring, local, first):
            taps = [ring[local:BLOCK, col_off // 2:col_off // 2 + 8, col_off % 2].reshape((BLOCK - local) * LANES, LANES) for col_off in range(4)]
            out = lax.dot_general(wo[...], jnp.concatenate(taps, axis=1), (((1,), (1,)), ((), ())), preferred_element_type=F32)
            for line in range(BLOCK - local):
                sums[first + line] = out[:, line * LANES:(line + 1) * LANES]

        chunk(-1)
        products(act_t[2], BLOCK - 2, 0)
        chunk(0)
        for step in range(STEPS):
            chunk(step + 1)
            products(act_t[step % 3], 0, step * BLOCK + 2)
            for line in range(step * BLOCK, step * BLOCK + BLOCK):
                flat[pl.ds(line, 8, stride=SLAB), :] = sums[line][0:8] + sums[line + 1][8:SUB] + sums[line + 2][SUB:SUB + 8]
        for channel in range(3):
            lines = [flat[pl.ds((3 * out_col + channel) * SLAB, SLAB), :] for out_col in range(2)]
            values = jnp.concatenate(lines, axis=1)
            total = jnp.zeros((LANES, 2 * SLAB), F32)
            for _ in range(3):
                term = values.astype(BF16)
                values = values - term.astype(F32)
                blank_half = jnp.zeros_like(term)
                spread = jnp.concatenate([jnp.concatenate([term, blank_half], axis=1), jnp.concatenate([blank_half, term], axis=1)], axis=0)
                total = total + lax.dot_general(order[...], spread, (((1,), (1,)), ((), ())), preferred_element_type=F32)
            image[pl.ds(g * 8, 8), channel] = total.reshape(8, SUB, 2 * SLAB)
        return carry

    lax.fori_loop(0, 2, out_conv, 0)


def solution(mesh):
    rows_n = mesh.shape["sy"]
    cols_n = mesh.shape["sx"]
    tile_spec = P("dp", "sy", "sx", None)
    replicated = P()
    dma = pltpu.SemaphoreType.DMA

    def local_decode(act_in, norm_first, w_first, w_short, norm_rest, w_rest, bias_rest, w_out, bias_out):
        vmem = pl.BlockSpec(memory_space=pltpu.VMEM)
        anywhere = pl.BlockSpec(memory_space=pl.ANY)
        planes = pl.pallas_call(
            functools.partial(kernel, rows_n, cols_n),
            out_shape=jax.ShapeDtypeStruct((SUB, 3, SUB, 2 * SLAB), F32),
            in_specs=[anywhere, vmem, anywhere, anywhere, vmem, anywhere, vmem, vmem],
            out_specs=vmem,
            scratch_shapes=[
                pltpu.VMEM((8 * SLAB, LANES), F32),
                pltpu.VMEM((LANES, 2 * WIDE), BF16),
                pltpu.VMEM((8, LANES), F32),
                pltpu.VMEM((DEPTH, 2, 8, CHUNK, SUB, WIDE), BF16),
                pltpu.VMEM((2, SLAB, 8, 2, SUB, WIDE), BF16),
                pltpu.VMEM((2, SLAB, 8, 2, SUB, LANES), BF16),
                pltpu.VMEM((2, SLAB, 8, 2, SUB, LANES), BF16),
                *[pltpu.VMEM((BLOCK, 9, 2, SUB, WIDE), BF16)] * 3,
                *[pltpu.VMEM((BLOCK, 9, 2, SUB, LANES), BF16)] * 3,
                pltpu.VMEM((3, 4, WIDE, WIDE), BF16),
                pltpu.VMEM((2, WIDE, WIDE), BF16),
                pltpu.VMEM((5, 3, 4, LANES, WIDE), BF16),
                pltpu.VMEM((32, 4 * LANES), BF16),
                pltpu.VMEM((WIDE, WIDE), BF16),
                pltpu.VMEM((512, LANES), BF16),
                pltpu.VMEM((WIDE, LANES), BF16),
                pltpu.VMEM((LANES, 512), BF16),
                pltpu.VMEM((LANES, WIDE), BF16),
                pltpu.VMEM((1, 2, 2, SLAB, SUB, WIDE), BF16),
                pltpu.VMEM((1, 2, 2, 8, 2, SUB, WIDE), BF16),
                pltpu.VMEM((1, 2, 2, 2, SUB, WIDE), BF16),
                pltpu.VMEM((2, 2, 2, SLAB, SUB, LANES), BF16),
                pltpu.VMEM((2, 2, 2, 8, 2, SUB, LANES), BF16),
                pltpu.VMEM((2, 2, 2, 2, SUB, LANES), BF16),
                pltpu.VMEM((2, 2, rows_n * cols_n, 8, LANES), F32),
                dma((DEPTH, 2)),
                dma((3, 2)),
                dma((2, 2, 2)),
                dma((2, 2, 2)),
                dma((2, 2, 2)),
                dma((2, 2, 2)),
                dma((2, 2, 2, 2)),
                dma((2, 2, 2, 2)),
                dma((2, 2)),
                dma((2, 2)),
            ],
            compiler_params=pltpu.CompilerParams(collective_id=0, has_side_effects=True, vmem_limit_bytes=62 << 20),
            name="decode",
        )(act_in, norm_first, w_first, w_short, norm_rest, w_rest, bias_rest, jnp.transpose(w_out, (0, 1, 3, 2)))
        return jnp.transpose(planes, (0, 3, 2, 1)) + bias_out.astype(F32)

    return jax.shard_map(local_decode, mesh=mesh, in_specs=(tile_spec, replicated, replicated, replicated, replicated, replicated, replicated, replicated, replicated), out_specs=tile_spec, check_vma=False)
```

```python
import functools

import jax
import jax.numpy as jnp
from jax import lax
from jax.experimental import pallas as pl
from jax.experimental.pallas import tpu as pltpu
from jax.sharding import PartitionSpec as P

GROUPS = 32
GN_EPS = 1e-6
MESH = pl.DeviceIdType.MESH
F32 = jnp.float32
LANES = 128
WIDE = 256
SUB = 16
SIDE = 512
DEEP = 1024
PAIR = (0, 1)
BF16 = jnp.bfloat16
SLAB = 48
BLOCK = 8
STEPS = SLAB // BLOCK
EARLY = 4
CHUNK = 4
DEPTH = 8
CHUNKS = SLAB // CHUNK


def exact_rows(values):
    high = values.astype(BF16).astype(F32)
    rest = values - high
    mid = rest.astype(BF16).astype(F32)
    low = rest - mid
    return jnp.concatenate([high, mid, low, jnp.zeros_like(low)], axis=0).astype(BF16)


def exact_dot(values, ones):
    out = jnp.dot(exact_rows(values), ones, preferred_element_type=F32)
    return (out[0:8] + out[8:SUB]) + out[SUB:24]


def group_matrix(channels, transposed):
    per_group = channels // GROUPS
    shape = (LANES, 2 * channels) if transposed else (2 * channels, LANES)
    chan = lax.broadcasted_iota(jnp.int32, shape, 1 if transposed else 0)
    lane = lax.broadcasted_iota(jnp.int32, shape, 0 if transposed else 1)
    target = jnp.where(chan < channels, chan // per_group, GROUPS + (chan - channels) // per_group)
    return jnp.where(target == lane, 1.0, 0.0).astype(BF16)


def kernel(rows_n, cols_n, act_in, norm_first, w_first, w_short, norm_rest, w_rest, bias_rest, w_out, image,
           flat, order, bias_f, stage, raw_a, raw_t, raw_h, act_a0, act_a1, act_a2, act_t0, act_t1, act_t2, wf, wfs, ws, wr, wrs, wo, perm, sum_a, sum_t, cast_a, cast_t,
           col_a, row_a, cor_a, col_t, row_t, cor_t, slots,
           in_sem, wt_sem, col_send, col_recv, row_send, row_recv, cor_send, cor_recv, stat_send, stat_recv):
    peers = rows_n * cols_n
    act_a = (act_a0, act_a1, act_a2)
    act_t = (act_t0, act_t1, act_t2)
    my_x = lax.axis_index("sx")
    my_y = lax.axis_index("sy")
    me = my_x * rows_n + my_y
    has_side = (my_x > 0, my_x < cols_n - 1)
    has_end = (my_y > 0, my_y < rows_n - 1)
    count = float(rows_n * cols_n * 2 * SLAB * SUB)

    def at(dx, dy):
        return {"sx": my_x + dx, "sy": my_y + dy}

    def peer(index):
        return {"sx": index // rows_n, "sy": lax.rem(index, rows_n)}

    def col_copy(raw, col, par, g, side, start, size):
        src = raw.at[g, pl.ds(start, size), 0 if side == 0 else 7, side]
        dst = col.at[par, g, 1 - side, pl.ds(start, size)]
        return pltpu.make_async_remote_copy(src, dst, col_send.at[par, g, side], col_recv.at[par, g, 1 - side], device_id=at(2 * side - 1, 0), device_id_type=MESH)

    def row_copy(raw, row, par, g, end):
        src = raw.at[g, 0 if end == 0 else SLAB - 1]
        return pltpu.make_async_remote_copy(src, row.at[par, g, 1 - end], row_send.at[par, g, end], row_recv.at[par, g, 1 - end], device_id=at(0, 2 * end - 1), device_id_type=MESH)

    def cor_copy(raw, cor, par, g, end, side):
        src = raw.at[g, 0 if end == 0 else SLAB - 1, 0 if side == 0 else 7, side]
        return pltpu.make_async_remote_copy(src, cor.at[par, g, 1 - end, 1 - side], cor_send.at[par, g, end, side], cor_recv.at[par, g, 1 - end, 1 - side], device_id=at(2 * side - 1, 2 * end - 1), device_id_type=MESH)

    def stat_copy(par, g, offset):
        return pltpu.make_async_remote_copy(slots.at[par, g, me], slots.at[par, g, me], stat_send.at[par, g], stat_recv.at[par, g], device_id=peer(lax.rem(me + offset, peers)), device_id_type=MESH)

    def send_cols(raw, col, par, g, start, size):
        for side in PAIR:
            @pl.when(has_side[side])
            def _():
                col_copy(raw, col, par, g, side, start, size).start()

    def send_ends(raw, row, cor, par, g):
        for end in PAIR:
            @pl.when(has_end[end])
            def _():
                row_copy(raw, row, par, g, end).start()
            for side in PAIR:
                @pl.when(jnp.logical_and(has_end[end], has_side[side]))
                def _():
                    cor_copy(raw, cor, par, g, end, side).start()

    def send_sums(par, g, message):
        slots[par, g, me] = message

        def one(offset, carry):
            stat_copy(par, g, offset).start()
            return carry

        lax.fori_loop(1, peers, one, 0)

    def finish_exchange(raw, col, row, cor, par, g):
        for side in PAIR:
            @pl.when(has_side[side])
            def _():
                col_copy(raw, col, par, g, side, 0, SLAB).wait_send()
                col_copy(raw, col, par, g, 1 - side, 0, SLAB).wait_recv()
        for end in PAIR:
            @pl.when(has_end[end])
            def _():
                row_copy(raw, row, par, g, end).wait_send()
                row_copy(raw, row, par, g, 1 - end).wait_recv()
            for side in PAIR:
                @pl.when(jnp.logical_and(has_end[end], has_side[side]))
                def _():
                    cor_copy(raw, cor, par, g, end, side).wait_send()
                    cor_copy(raw, cor, par, g, 1 - end, 1 - side).wait_recv()
        arrived = slots.at[par, g, pl.ds(0, peers - 1)]
        done = pltpu.make_async_remote_copy(arrived, arrived, stat_send.at[par, g], stat_recv.at[par, g], device_id=peer(lax.rem(me + 1, peers)), device_id_type=MESH)
        done.wait_send()
        done.wait_recv()

    def message_of(sum_one, sum_two, ones):
        both = jnp.concatenate([sum_one[0:8] + sum_one[8:SUB], sum_two[0:8] + sum_two[8:SUB]], axis=1)
        return exact_dot(both, ones)

    def half_affine(par, g, spread, norm_pair, channels):
        totals = slots[par, g, 0]
        for index in range(1, peers):
            totals = totals + slots[par, g, index]
        sums = exact_dot(totals, spread)
        inv_count = 1.0 / (count * (channels // GROUPS))
        mean = sums[:, :channels] * inv_count
        inv_std = lax.rsqrt(sums[:, channels:] * inv_count - mean * mean + GN_EPS)
        pair = norm_pair.astype(F32)
        scale = inv_std * pair[0:1]
        shift = pair[1:2] - mean * scale
        scale, shift = scale * 0.5, shift * 0.5
        return jnp.concatenate([scale, scale], axis=0), jnp.concatenate([shift, shift], axis=0)

    def activate(values, scale, shift):
        half = values.astype(F32) * scale + shift
        return half + half * jnp.tanh(half)

    def activation(raw, act, col, row, cor, par, g, scale, shift):
        def rows(ring, local, first, size):
            out = activate(raw[g, first:first + size], scale, shift).astype(BF16)
            ring[local:local + size, 0:8, 1] = out[:, :, 0]
            ring[local:local + size, 1:9, 0] = out[:, :, 1]
            for side in PAIR:
                edge = activate(col[par, g, side, first:first + size], scale, shift)
                ring[local:local + size, 8 * side, side] = jnp.where(has_side[side], edge, 0.0).astype(BF16)

        def outer_row(ring, local, end):
            inner = SLAB - 1 if end == 0 else 0
            low, high = slice(0, 8), slice(8, SUB)
            own, far = (low, high) if end == 0 else (high, low)

            def join(mine, theirs, mine_present, theirs_present):
                near = activate(mine.astype(F32)[..., own, :], scale[0:8], shift[0:8])
                away = activate(theirs.astype(F32)[..., far, :], scale[0:8], shift[0:8])
                if mine_present is not None:
                    near = jnp.where(mine_present, near, 0.0)
                away = jnp.where(theirs_present, away, 0.0)
                return jnp.concatenate([away, near] if end == 0 else [near, away], axis=-2).astype(BF16)

            line = join(raw[g, inner], row[par, g, end], None, has_end[end])
            ring[local, 0:8, 1] = line[:, 0]
            ring[local, 1:9, 0] = line[:, 1]
            for side in PAIR:
                both = jnp.logical_and(has_end[end], has_side[side])
                ring[local, 8 * side, side] = join(col[par, g, side, inner], cor[par, g, end, side], has_side[side], both)

        def chunk(index):
            ring = act[index % 3]
            if index < 0:
                outer_row(ring, BLOCK - 2, 0)
                rows(ring, BLOCK - 1, 0, 1)
            elif index < STEPS - 1:
                rows(ring, 0, index * BLOCK + 1, BLOCK)
            elif index == STEPS - 1:
                rows(ring, 0, index * BLOCK + 1, BLOCK - 1)
                outer_row(ring, BLOCK - 1, 1)

        return chunk

    def line_of(act, index, place, col_off):
        ring, local = (act[index % 3], place - 2) if place >= 2 else (act[(index - 1) % 3], place + BLOCK - 2)
        return ring[local, col_off // 2:col_off // 2 + 8, col_off % 2]

    def windows(act, index, places, col_off, channels):
        lines = [line_of(act, index, place, col_off).reshape(LANES, channels) for place in places]
        return jnp.concatenate(lines, axis=0)

    def side_product(act, index, col_off, channels, weights):
        taps = [windows(act, index, range(place, place + BLOCK, 2), col_off, channels) for place in range(4)]
        out = jnp.dot(jnp.concatenate(taps, axis=1), weights, preferred_element_type=F32).reshape(BLOCK // 2, LANES, WIDE)
        return jnp.stack([out[..., :LANES], out[..., LANES:]], axis=1).reshape(BLOCK * LANES, LANES)

    def convolve(act, chunk, channels, weights, bias, dst, col, row, cor, par, g, extra=None, residual=None):
        bias_pair = jnp.concatenate([bias, bias], axis=1)
        sum_one = sum_two = jnp.zeros((SUB, WIDE), F32)
        chunk(-1)
        chunk(0)
        for step in range(STEPS):
            span = slice(step * BLOCK, step * BLOCK + BLOCK)
            taps = [windows(act, step, range(row_off, row_off + BLOCK), col_off, channels) for row_off in range(3) for col_off in (1, 2)]
            if extra is not None:
                taps = taps + extra(span)
            middle, left, right = weights()
            sides = [side_product(act, step, 0, channels, left), side_product(act, step, 3, channels, right)]
            out = jnp.dot(jnp.concatenate(taps, axis=1), middle, preferred_element_type=F32) + bias_pair
            out = out + jnp.concatenate(sides, axis=1)
            if residual is not None:
                kept = residual[g, span].astype(F32)
                kept = jnp.concatenate([kept[:, :, 0], kept[:, :, 1]], axis=-1)
                out = out + kept.reshape(BLOCK * LANES, WIDE)
            rounded = out.astype(BF16)
            wide = rounded.astype(F32).reshape(BLOCK * 8, SUB, WIDE)
            sum_one = sum_one + jnp.sum(wide, axis=0)
            sum_two = sum_two + jnp.sum(wide * wide, axis=0)
            tiles = rounded.reshape(BLOCK, 8, SUB, WIDE)
            dst[g, span, :, 0] = tiles[..., :LANES]
            dst[g, span, :, 1] = tiles[..., LANES:]
            chunk(step + 1)
            if step == EARLY - 1:
                send_cols(dst, col, par, g, 0, EARLY * BLOCK)
        send_sums(par, g, message_of(sum_one[:, :LANES] + sum_one[:, LANES:], sum_two[:, :LANES] + sum_two[:, LANES:], sum_t[...]))
        send_ends(dst, row, cor, par, g)
        send_cols(dst, col, par, g, EARLY * BLOCK, SLAB - EARLY * BLOCK)

    def input_copy(g, chunk, half):
        index = g * CHUNKS + chunk
        slot = lax.rem(index, DEPTH)
        src = act_in.at[pl.ds(g * 8, 8), pl.ds(half * SLAB + chunk * CHUNK, CHUNK)]
        return pltpu.make_async_copy(src, stage.at[slot, half], in_sem.at[slot, half])

    for early in range(DEPTH):
        for half in PAIR:
            input_copy(0, early, half).start()

    barrier = pltpu.get_barrier_semaphore()

    def greet(offset, carry):
        pl.semaphore_signal(barrier, inc=1, device_id=peer(lax.rem(me + offset, peers)), device_id_type=MESH)
        return carry

    lax.fori_loop(1, peers, greet, 0)

    out_row = lax.broadcasted_iota(jnp.int32, (WIDE, WIDE), 0)
    in_row = lax.broadcasted_iota(jnp.int32, (WIDE, WIDE), 1)
    swapped = jnp.logical_and(out_row // SUB == in_row % SUB, out_row % SUB == in_row // SUB)
    perm[...] = jnp.where(swapped, 1.0, 0.0).astype(BF16)
    shape = (LANES, 2 * WIDE)
    target = lax.broadcasted_iota(jnp.int32, shape, 0)
    lane = lax.broadcasted_iota(jnp.int32, shape, 1)
    half_at, col_at, pair_at = lane // WIDE, lane // LANES % 2, lane // SUB % 8
    wanted = jnp.logical_and(lane // 8 % 2 == half_at, target == lane % 8 * SUB + 2 * pair_at + col_at)
    order[...] = jnp.where(wanted, 1.0, 0.0).astype(BF16)
    bias_f[0:7] = bias_rest[...].astype(F32)
    sum_a[...] = group_matrix(WIDE, False)
    sum_t[...] = group_matrix(LANES, False)
    cast_a[...] = group_matrix(WIDE, True)
    cast_t[...] = group_matrix(LANES, True)
    for side in PAIR:
        wfs[side, 3, :, 0:LANES] = jnp.zeros((WIDE, LANES), BF16)
        wfs[side, 0, :, LANES:WIDE] = jnp.zeros((WIDE, LANES), BF16)
        for index in range(5):
            wrs[index, side, 3, :, 0:LANES] = jnp.zeros((LANES, LANES), BF16)
            wrs[index, side, 0, :, LANES:WIDE] = jnp.zeros((LANES, LANES), BF16)
    ws[0, :, LANES:WIDE] = jnp.zeros((WIDE, LANES), BF16)
    ws[1, :, 0:LANES] = jnp.zeros((WIDE, LANES), BF16)

    def weight_copies(first):
        copies = []
        for out_col in PAIR:
            lanes = pl.ds(out_col * LANES, LANES)
            inner = pl.ds(1 - out_col, 2)
            rows_at = pl.ds(out_col, 3)
            if first:
                copies.append(pltpu.make_async_copy(w_first.at[:, inner], wf.at[:, :, :, lanes], wt_sem.at[0, out_col, 0]))
            else:
                copies.append(pltpu.make_async_copy(w_short, ws.at[out_col, :, lanes], wt_sem.at[1, out_col, 0]))
                copies.append(pltpu.make_async_copy(w_rest.at[:, :, inner], wr.at[:, :, :, :, lanes], wt_sem.at[2, out_col, 0]))
            for side in PAIR:
                if first:
                    copies.append(pltpu.make_async_copy(w_first.at[:, 2 * side], wfs.at[side, rows_at, :, lanes], wt_sem.at[0, out_col, 1 + side]))
                else:
                    copies.append(pltpu.make_async_copy(w_rest.at[:, :, 2 * side], wrs.at[:, side, rows_at, :, lanes], wt_sem.at[2, out_col, 1 + side]))
        return copies

    for copy in weight_copies(True):
        copy.start()

    blank = jnp.zeros((3, LANES), F32)
    blocks = []
    for row_off in range(3):
        parts = []
        for col_off in range(4):
            taps = [w_out[row_off, col_off - out_col].astype(F32) if 0 <= col_off - out_col < 3 else blank for out_col in PAIR]
            parts.append(jnp.concatenate(taps + [blank[0:2]], axis=0))
        blocks.append(jnp.concatenate(parts, axis=1))
    blocks.append(jnp.zeros_like(blocks[0]))
    wo[...] = jnp.concatenate(blocks, axis=0).astype(BF16)

    def load_group(g, carry):
        def body(chunk, sums):
            sum_one, sum_two = sums
            index = g * CHUNKS + chunk
            slot = lax.rem(index, DEPTH)
            for half in PAIR:
                input_copy(g, chunk, half).wait()
            for line in range(CHUNK):
                tile = stage[slot, :, :, line].reshape(WIDE, WIDE)
                out = jnp.dot(perm[...], tile, preferred_element_type=F32)
                cube = out.reshape(SUB, SUB, WIDE)
                sum_one = sum_one + jnp.sum(cube, axis=0)
                sum_two = sum_two + jnp.sum(cube * cube, axis=0)
                raw_a[g, chunk * CHUNK + line] = out.astype(BF16).reshape(8, 2, SUB, WIDE)
            later = index + DEPTH

            @pl.when(later < 2 * CHUNKS)
            def _():
                next_g = later // CHUNKS
                for half in PAIR:
                    input_copy(next_g, later - next_g * CHUNKS, half).start()

            @pl.when(index == 1)
            def _():
                pl.semaphore_wait(barrier, peers - 1)

            @pl.when(chunk > 0)
            def _():
                send_cols(raw_a, col_a, 0, g, (chunk - 1) * CHUNK, CHUNK)

            return sum_one, sum_two

        zero = jnp.zeros((SUB, WIDE), F32)
        sum_one, sum_two = lax.fori_loop(0, CHUNKS, body, (zero, zero))
        send_sums(0, g, message_of(sum_one, sum_two, sum_a[...]))
        send_cols(raw_a, col_a, 0, g, SLAB - CHUNK, CHUNK)
        send_ends(raw_a, row_a, cor_a, 0, g)
        return carry

    lax.fori_loop(0, 2, load_group, 0)
    for copy in weight_copies(False):
        copy.start()
    for copy in weight_copies(True):
        copy.wait()

    def bias_row(index):
        return bias_f[pl.ds(index, 1)]

    def first_conv(g, carry):
        finish_exchange(raw_a, col_a, row_a, cor_a, 0, g)
        scale, shift = half_affine(0, g, cast_a[...], norm_first[...], WIDE)
        chunk = activation(raw_a, act_a, col_a, row_a, cor_a, 0, g, scale, shift)
        convolve(act_a, chunk, WIDE, lambda: (wf[...].reshape(1536, WIDE), wfs[0].reshape(DEEP, WIDE), wfs[1].reshape(DEEP, WIDE)), bias_row(0), raw_t, col_t, row_t, cor_t, 1, g)
        return carry

    lax.fori_loop(0, 2, first_conv, 0)
    for copy in weight_copies(False):
        copy.wait()

    def layer(src, norm_at, weights, bias, dst, par, g, **more):
        finish_exchange(src, col_t, row_t, cor_t, par, g)
        scale, shift = half_affine(par, g, cast_t[...], norm_rest[norm_at], LANES)
        chunk = activation(src, act_t, col_t, row_t, cor_t, par, g, scale, shift)
        if weights is not None:
            convolve(act_t, chunk, LANES, weights, bias, dst, col_t, row_t, cor_t, 1 - par, g, **more)
        return chunk

    def side_weights(index):
        return wrs[index, 0].reshape(SIDE, WIDE), wrs[index, 1].reshape(SIDE, WIDE)

    def shortcut_conv(g, carry):
        def extra(span):
            return [raw_a[g, span, :, which].reshape(BLOCK * LANES, WIDE) for which in range(2)]

        def weights():
            return (jnp.concatenate([wr[0].reshape(768, WIDE), ws[...].reshape(SIDE, WIDE)], axis=0), *side_weights(0))

        layer(raw_t, 0, weights, bias_row(1) + bias_row(6), raw_h, 1, g, extra=extra)
        return carry

    lax.fori_loop(0, 2, shortcut_conv, 0)

    def resnet(res, carry):
        base = 2 * res + 1

        def first_half(g, inner):
            layer(raw_h, base, lambda: (wr[base].reshape(768, WIDE), *side_weights(base)), bias_row(base + 1), raw_t, 0, g)
            return inner

        def second_half(g, inner):
            layer(raw_t, base + 1, lambda: (wr[base + 1].reshape(768, WIDE), *side_weights(base + 1)), bias_row(base + 2), raw_h, 1, g, residual=raw_h)
            return inner

        lax.fori_loop(0, 2, first_half, 0)
        lax.fori_loop(0, 2, second_half, 0)
        return carry

    lax.fori_loop(0, 2, resnet, 0)

    def out_conv(g, carry):
        chunk = layer(raw_h, 5, None, None, None, 0, g)
        sums = {}

        def products(ring, local, first):
            taps = [ring[local:BLOCK, col_off // 2:col_off // 2 + 8, col_off % 2].reshape((BLOCK - local) * LANES, LANES) for col_off in range(4)]
            out = lax.dot_general(wo[...], jnp.concatenate(taps, axis=1), (((1,), (1,)), ((), ())), preferred_element_type=F32)
            for line in range(BLOCK - local):
                sums[first + line] = out[:, line * LANES:(line + 1) * LANES]

        chunk(-1)
        products(act_t[2], BLOCK - 2, 0)
        chunk(0)
        for step in range(STEPS):
            chunk(step + 1)
            products(act_t[step % 3], 0, step * BLOCK + 2)
            for line in range(step * BLOCK, step * BLOCK + BLOCK):
                flat[pl.ds(line, 8, stride=SLAB), :] = sums[line][0:8] + sums[line + 1][8:SUB] + sums[line + 2][SUB:SUB + 8]
        for channel in range(3):
            lines = [flat[pl.ds((3 * out_col + channel) * SLAB, SLAB), :] for out_col in PAIR]
            values = jnp.concatenate(lines, axis=1)
            total = jnp.zeros((LANES, 2 * SLAB), F32)
            for _ in range(3):
                term = values.astype(BF16)
                values = values - term.astype(F32)
                blank_half = jnp.zeros_like(term)
                spread = jnp.concatenate([jnp.concatenate([term, blank_half], axis=1), jnp.concatenate([blank_half, term], axis=1)], axis=0)
                total = total + lax.dot_general(order[...], spread, (((1,), (1,)), ((), ())), preferred_element_type=F32)
            image[pl.ds(g * 8, 8), channel] = total.reshape(8, SUB, 2 * SLAB)
        return carry

    lax.fori_loop(0, 2, out_conv, 0)


def solution(mesh):
    rows_n = mesh.shape["sy"]
    cols_n = mesh.shape["sx"]
    tile_spec = P("dp", "sy", "sx", None)
    replicated = P()
    dma = pltpu.SemaphoreType.DMA

    def local_decode(act_in, norm_first, w_first, w_short, norm_rest, w_rest, bias_rest, w_out, bias_out):
        vmem = pl.BlockSpec(memory_space=pltpu.VMEM)
        anywhere = pl.BlockSpec(memory_space=pl.ANY)
        planes = pl.pallas_call(
            functools.partial(kernel, rows_n, cols_n),
            out_shape=jax.ShapeDtypeStruct((SUB, 3, SUB, 2 * SLAB), F32),
            in_specs=[anywhere, vmem, anywhere, anywhere, vmem, anywhere, vmem, vmem],
            out_specs=vmem,
            scratch_shapes=[
                pltpu.VMEM((8 * SLAB, LANES), F32),
                pltpu.VMEM((LANES, 2 * WIDE), BF16),
                pltpu.VMEM((8, LANES), F32),
                pltpu.VMEM((DEPTH, 2, 8, CHUNK, SUB, WIDE), BF16),
                pltpu.VMEM((2, SLAB, 8, 2, SUB, WIDE), BF16),
                pltpu.VMEM((2, SLAB, 8, 2, SUB, LANES), BF16),
                pltpu.VMEM((2, SLAB, 8, 2, SUB, LANES), BF16),
                *[pltpu.VMEM((BLOCK, 9, 2, SUB, WIDE), BF16)] * 3,
                *[pltpu.VMEM((BLOCK, 9, 2, SUB, LANES), BF16)] * 3,
                pltpu.VMEM((3, 2, WIDE, WIDE), BF16),
                pltpu.VMEM((2, 4, WIDE, WIDE), BF16),
                pltpu.VMEM((2, WIDE, WIDE), BF16),
                pltpu.VMEM((5, 3, 2, LANES, WIDE), BF16),
                pltpu.VMEM((5, 2, 4, LANES, WIDE), BF16),
                pltpu.VMEM((32, 4 * LANES), BF16),
                pltpu.VMEM((WIDE, WIDE), BF16),
                pltpu.VMEM((SIDE, LANES), BF16),
                pltpu.VMEM((WIDE, LANES), BF16),
                pltpu.VMEM((LANES, SIDE), BF16),
                pltpu.VMEM((LANES, WIDE), BF16),
                pltpu.VMEM((1, 2, 2, SLAB, SUB, WIDE), BF16),
                pltpu.VMEM((1, 2, 2, 8, 2, SUB, WIDE), BF16),
                pltpu.VMEM((1, 2, 2, 2, SUB, WIDE), BF16),
                pltpu.VMEM((2, 2, 2, SLAB, SUB, LANES), BF16),
                pltpu.VMEM((2, 2, 2, 8, 2, SUB, LANES), BF16),
                pltpu.VMEM((2, 2, 2, 2, SUB, LANES), BF16),
                pltpu.VMEM((2, 2, rows_n * cols_n, 8, LANES), F32),
                dma((DEPTH, 2)),
                dma((3, 2, 3)),
                dma((2, 2, 2)),
                dma((2, 2, 2)),
                dma((2, 2, 2)),
                dma((2, 2, 2)),
                dma((2, 2, 2, 2)),
                dma((2, 2, 2, 2)),
                dma((2, 2)),
                dma((2, 2)),
            ],
            compiler_params=pltpu.CompilerParams(collective_id=0, has_side_effects=True, vmem_limit_bytes=62 << 20),
            name="decode",
        )(act_in, norm_first, w_first, w_short, norm_rest, w_rest, bias_rest, jnp.transpose(w_out, (0, 1, 3, 2)))
        return jnp.transpose(planes, (0, 3, 2, 1)) + bias_out.astype(F32)

    return jax.shard_map(local_decode, mesh=mesh, in_specs=(tile_spec, replicated, replicated, replicated, replicated, replicated, replicated, replicated, replicated), out_specs=tile_spec, check_vma=False)
```

```python
import functools

import jax
import jax.numpy as jnp
from jax import lax
from jax.experimental import pallas as pl
from jax.experimental.pallas import tpu as pltpu
from jax.sharding import PartitionSpec as P

GROUPS = 32
GN_EPS = 1e-6
MESH = pl.DeviceIdType.MESH
F32 = jnp.float32
LANES = 128
WIDE = 256
SUB = 16
SIDE = 512
DEEP = 1024
PAIR = (0, 1)
ZERO = 0.0
BF16 = jnp.bfloat16
SLAB = 48
BLOCK = 8
STEPS = SLAB // BLOCK
EARLY = 4
SENT = 24
CHUNK = 4
DEPTH = 8
CHUNKS = SLAB // CHUNK


def over_groups(body):
    lax.fori_loop(0, 2, body, 0)


def exact_rows(values):
    high = values.astype(BF16).astype(F32)
    rest = values - high
    mid = rest.astype(BF16).astype(F32)
    low = rest - mid
    return jnp.concatenate([high, mid, low, jnp.zeros_like(low)], axis=0).astype(BF16)


def exact_dot(values, ones):
    out = jnp.dot(exact_rows(values), ones, preferred_element_type=F32)
    return (out[0:8] + out[8:SUB]) + out[SUB:24]


def group_matrix(channels, transposed):
    per_group = channels // GROUPS
    shape = (LANES, 2 * channels) if transposed else (2 * channels, LANES)
    chan = lax.broadcasted_iota(jnp.int32, shape, 1 if transposed else 0)
    lane = lax.broadcasted_iota(jnp.int32, shape, 0 if transposed else 1)
    target = jnp.where(chan < channels, chan // per_group, GROUPS + (chan - channels) // per_group)
    return jnp.where(target == lane, 1.0, 0.0).astype(BF16)


def kernel(rows_n, cols_n, act_in, norm_first, w_first, w_short, norm_rest, w_rest, bias_rest, w_out, image,
           flat, order, bias_f, stage, raw_a, raw_t, raw_h, act_a0, act_a1, act_a2, act_t0, act_t1, act_t2, wf, wfs, ws, wr, wrs, wo, perm, sum_a, sum_t, cast_a, cast_t,
           col_a, row_a, cor_a, col_t, row_t, cor_t, slots,
           in_sem, wt_sem, col_send, col_recv, row_send, row_recv, cor_send, cor_recv, stat_send, stat_recv, ready):
    peers = rows_n * cols_n
    act_a = (act_a0, act_a1, act_a2)
    act_t = (act_t0, act_t1, act_t2)
    my_x = lax.axis_index("sx")
    my_y = lax.axis_index("sy")
    me = my_x * rows_n + my_y
    has_side = (my_x > 0, my_x < cols_n - 1)
    has_end = (my_y > 0, my_y < rows_n - 1)
    count = float(rows_n * cols_n * 2 * SLAB * SUB)

    def at(dx, dy):
        return {"sx": my_x + dx, "sy": my_y + dy}

    def peer(index):
        return {"sx": index // rows_n, "sy": lax.rem(index, rows_n)}

    def col_copy(raw, col, par, g, side, start, size):
        src = raw.at[g, pl.ds(start, size), 0 if side == 0 else 7, side]
        dst = col.at[par, g, 1 - side, pl.ds(start, size)]
        return pltpu.make_async_remote_copy(src, dst, col_send.at[par, g, side], col_recv.at[par, g, 1 - side], device_id=at(2 * side - 1, 0), device_id_type=MESH)

    def row_copy(raw, row, par, g, end):
        src = raw.at[g, 0 if end == 0 else SLAB - 1]
        return pltpu.make_async_remote_copy(src, row.at[par, g, 1 - end], row_send.at[par, g, end], row_recv.at[par, g, 1 - end], device_id=at(0, 2 * end - 1), device_id_type=MESH)

    def cor_copy(raw, cor, par, g, end, side):
        src = raw.at[g, 0 if end == 0 else SLAB - 1, 0 if side == 0 else 7, side]
        return pltpu.make_async_remote_copy(src, cor.at[par, g, 1 - end, 1 - side], cor_send.at[par, g, end, side], cor_recv.at[par, g, 1 - end, 1 - side], device_id=at(2 * side - 1, 2 * end - 1), device_id_type=MESH)

    def stat_copy(par, g, offset):
        return pltpu.make_async_remote_copy(slots.at[par, g, me], slots.at[par, g, me], stat_send.at[par, g], stat_recv.at[par, g], device_id=peer(lax.rem(me + offset, peers)), device_id_type=MESH)

    def send_cols(raw, col, par, g, start, size):
        for side in PAIR:
            @pl.when(has_side[side])
            def _():
                col_copy(raw, col, par, g, side, start, size).start()

    def send_ends(raw, row, cor, par, g):
        for end in PAIR:
            @pl.when(has_end[end])
            def _():
                row_copy(raw, row, par, g, end).start()
            for side in PAIR:
                @pl.when(jnp.logical_and(has_end[end], has_side[side]))
                def _():
                    cor_copy(raw, cor, par, g, end, side).start()

    def send_sums(par, g, message):
        slots[par, g, me] = message

        for offset in sorted(range(1, peers), key=lambda offset: -min(offset, peers - offset)):
            stat_copy(par, g, offset).start()

    def finish_exchange(raw, col, row, cor, par, g):
        for side in PAIR:
            @pl.when(has_side[side])
            def _():
                col_copy(raw, col, par, g, side, 0, SLAB).wait_send()
                col_copy(raw, col, par, g, 1 - side, 0, SLAB).wait_recv()
        for end in PAIR:
            @pl.when(has_end[end])
            def _():
                row_copy(raw, row, par, g, end).wait_send()
                row_copy(raw, row, par, g, 1 - end).wait_recv()
            for side in PAIR:
                @pl.when(jnp.logical_and(has_end[end], has_side[side]))
                def _():
                    cor_copy(raw, cor, par, g, end, side).wait_send()
                    cor_copy(raw, cor, par, g, 1 - end, 1 - side).wait_recv()
        arrived = slots.at[par, g, pl.ds(0, peers - 1)]
        done = pltpu.make_async_remote_copy(arrived, arrived, stat_send.at[par, g], stat_recv.at[par, g], device_id=peer(lax.rem(me + 1, peers)), device_id_type=MESH)
        done.wait_send()
        done.wait_recv()

    def message_of(sum_one, sum_two, ones):
        both = jnp.concatenate([sum_one[0:8] + sum_one[8:SUB], sum_two[0:8] + sum_two[8:SUB]], axis=1)
        return exact_dot(both, ones)

    def half_affine(par, g, spread, norm_pair, channels):
        totals = slots[par, g, 0]
        for index in range(1, peers):
            totals = totals + slots[par, g, index]
        sums = exact_dot(totals, spread)
        inv_count = 1.0 / (count * (channels // GROUPS))
        mean = sums[:, :channels] * inv_count
        inv_std = lax.rsqrt(sums[:, channels:] * inv_count - mean * mean + GN_EPS)
        pair = norm_pair.astype(F32)
        scale = inv_std * pair[0:1]
        shift = pair[1:2] - mean * scale
        scale, shift = scale * 0.5, shift * 0.5
        return jnp.concatenate([scale, scale], axis=0), jnp.concatenate([shift, shift], axis=0)

    def activate(values, scale, shift):
        half = values.astype(F32) * scale + shift
        return half + half * jnp.tanh(half)

    def activation(raw, act, col, row, cor, par, g, scale, shift):
        def rows(ring, local, first, size):
            out = activate(raw[g, first:first + size], scale, shift).astype(BF16)
            ring[local:local + size, 0:8, 1] = out[:, :, 0]
            ring[local:local + size, 1:9, 0] = out[:, :, 1]
            for side in PAIR:
                edge = activate(col[par, g, side, first:first + size], scale, shift)
                ring[local:local + size, 8 * side, side] = jnp.where(has_side[side], edge, ZERO).astype(BF16)

        def outer_row(ring, local, end):
            inner = SLAB - 1 if end == 0 else 0
            low, high = slice(0, 8), slice(8, SUB)
            own, far = (low, high) if end == 0 else (high, low)

            def join(mine, theirs, mine_present, theirs_present):
                near = activate(mine.astype(F32)[..., own, :], scale[0:8], shift[0:8])
                away = activate(theirs.astype(F32)[..., far, :], scale[0:8], shift[0:8])
                if mine_present is not None:
                    near = jnp.where(mine_present, near, ZERO)
                away = jnp.where(theirs_present, away, ZERO)
                return jnp.concatenate([away, near] if end == 0 else [near, away], axis=-2).astype(BF16)

            line = join(raw[g, inner], row[par, g, end], None, has_end[end])
            ring[local, 0:8, 1] = line[:, 0]
            ring[local, 1:9, 0] = line[:, 1]
            for side in PAIR:
                both = jnp.logical_and(has_end[end], has_side[side])
                ring[local, 8 * side, side] = join(col[par, g, side, inner], cor[par, g, end, side], has_side[side], both)

        def chunk(index):
            ring = act[index % 3]
            if index < 0:
                outer_row(ring, BLOCK - 2, 0)
                rows(ring, BLOCK - 1, 0, 1)
            elif index < STEPS - 1:
                rows(ring, 0, index * BLOCK + 1, BLOCK)
            elif index == STEPS - 1:
                rows(ring, 0, index * BLOCK + 1, BLOCK - 1)
                outer_row(ring, BLOCK - 1, 1)

        return chunk

    def line_of(act, index, place, col_off):
        ring, local = (act[index % 3], place - 2) if place >= 2 else (act[(index - 1) % 3], place + BLOCK - 2)
        return ring[local, col_off // 2:col_off // 2 + 8, col_off % 2]

    def windows(act, index, places, col_off, channels):
        lines = [line_of(act, index, place, col_off).reshape(LANES, channels) for place in places]
        return jnp.concatenate(lines, axis=0)

    def side_product(act, index, col_off, channels, weights):
        taps = [windows(act, index, range(place, place + BLOCK, 2), col_off, channels) for place in range(4)]
        out = jnp.dot(jnp.concatenate(taps, axis=1), weights, preferred_element_type=F32).reshape(BLOCK // 2, LANES, WIDE)
        return jnp.stack([out[..., :LANES], out[..., LANES:]], axis=1).reshape(BLOCK * LANES, LANES)

    def convolve(act, chunk, channels, weights, bias, dst, col, row, cor, par, g, extra=None, residual=None):
        bias_pair = jnp.concatenate([bias, bias], axis=1)
        sum_one = sum_two = jnp.zeros((SUB, WIDE), F32)
        chunk(-1)
        chunk(0)
        for step in range(STEPS):
            span = slice(step * BLOCK, step * BLOCK + BLOCK)
            taps = [windows(act, step, range(row_off, row_off + BLOCK), col_off, channels) for row_off in range(3) for col_off in (1, 2)]
            if extra is not None:
                taps = taps + extra(span)
            middle, left, right = weights()
            sides = [side_product(act, step, 0, channels, left), side_product(act, step, 3, channels, right)]
            out = jnp.dot(jnp.concatenate(taps, axis=1), middle, preferred_element_type=F32) + bias_pair
            out = out + jnp.concatenate(sides, axis=1)
            if residual is not None:
                kept = residual[g, span].astype(F32)
                kept = jnp.concatenate([kept[:, :, 0], kept[:, :, 1]], axis=-1)
                out = out + kept.reshape(BLOCK * LANES, WIDE)
            rounded = out.astype(BF16)
            wide = rounded.astype(F32).reshape(BLOCK * 8, SUB, WIDE)
            sum_one = sum_one + jnp.sum(wide, axis=0)
            sum_two = sum_two + jnp.sum(wide * wide, axis=0)
            tiles = rounded.reshape(BLOCK, 8, SUB, WIDE)
            dst[g, span, :, 0] = tiles[..., :LANES]
            dst[g, span, :, 1] = tiles[..., LANES:]
            chunk(step + 1)
            if step == EARLY - 1:
                send_cols(dst, col, par, g, 0, SENT)
        send_sums(par, g, message_of(sum_one[:, :LANES] + sum_one[:, LANES:], sum_two[:, :LANES] + sum_two[:, LANES:], sum_t[...]))
        send_ends(dst, row, cor, par, g)
        send_cols(dst, col, par, g, SENT, SLAB - SENT)

    def input_copy(g, chunk, half):
        index = g * CHUNKS + chunk
        slot = lax.rem(index, DEPTH)
        src = act_in.at[pl.ds(g * 8, 8), pl.ds(half * SLAB + chunk * CHUNK, CHUNK)]
        return pltpu.make_async_copy(src, stage.at[slot, half], in_sem.at[slot, half])

    for early in range(DEPTH):
        for half in PAIR:
            input_copy(0, early, half).start()

    barrier = pltpu.get_barrier_semaphore()

    beside = 1 + sum(flag.astype(jnp.int32) for flag in has_side)
    around = beside * (1 + sum(flag.astype(jnp.int32) for flag in has_end)) - 1

    def greet(semaphore):
        for side in PAIR:
            @pl.when(has_side[side])
            def _():
                pl.semaphore_signal(semaphore, inc=1, device_id=at(2 * side - 1, 0), device_id_type=MESH)
        for end in PAIR:
            @pl.when(has_end[end])
            def _():
                pl.semaphore_signal(semaphore, inc=1, device_id=at(0, 2 * end - 1), device_id_type=MESH)
            for side in PAIR:
                @pl.when(jnp.logical_and(has_end[end], has_side[side]))
                def _():
                    pl.semaphore_signal(semaphore, inc=1, device_id=at(2 * side - 1, 2 * end - 1), device_id_type=MESH)

    rounds = max(rows_n, cols_n) - 1
    greet(barrier)

    out_row = lax.broadcasted_iota(jnp.int32, (WIDE, WIDE), 0)
    in_row = lax.broadcasted_iota(jnp.int32, (WIDE, WIDE), 1)
    swapped = jnp.logical_and(out_row // SUB == in_row % SUB, out_row % SUB == in_row // SUB)
    perm[...] = jnp.where(swapped, 1.0, 0.0).astype(BF16)
    shape = (LANES, 2 * WIDE)
    target = lax.broadcasted_iota(jnp.int32, shape, 0)
    lane = lax.broadcasted_iota(jnp.int32, shape, 1)
    half_at, col_at, pair_at = lane // WIDE, lane // LANES % 2, lane // SUB % 8
    wanted = jnp.logical_and(lane // 8 % 2 == half_at, target == lane % 8 * SUB + 2 * pair_at + col_at)
    order[...] = jnp.where(wanted, 1.0, 0.0).astype(BF16)
    bias_f[0:7] = bias_rest[...].astype(F32)
    sum_a[...] = group_matrix(WIDE, False)
    sum_t[...] = group_matrix(LANES, False)
    cast_a[...] = group_matrix(WIDE, True)
    cast_t[...] = group_matrix(LANES, True)
    for side in PAIR:
        wfs[side, 3, :, 0:LANES] = jnp.zeros((WIDE, LANES), BF16)
        wfs[side, 0, :, LANES:WIDE] = jnp.zeros((WIDE, LANES), BF16)
        for index in range(5):
            wrs[index, side, 3, :, 0:LANES] = jnp.zeros((LANES, LANES), BF16)
            wrs[index, side, 0, :, LANES:WIDE] = jnp.zeros((LANES, LANES), BF16)
    ws[0, :, LANES:WIDE] = jnp.zeros((WIDE, LANES), BF16)
    ws[1, :, 0:LANES] = jnp.zeros((WIDE, LANES), BF16)

    def weight_copies(first):
        copies = []
        for out_col in PAIR:
            lanes = pl.ds(out_col * LANES, LANES)
            inner = pl.ds(1 - out_col, 2)
            rows_at = pl.ds(out_col, 3)
            if first:
                copies.append(pltpu.make_async_copy(w_first.at[:, inner], wf.at[:, :, :, lanes], wt_sem.at[0, out_col, 0]))
            else:
                copies.append(pltpu.make_async_copy(w_short, ws.at[out_col, :, lanes], wt_sem.at[1, out_col, 0]))
                copies.append(pltpu.make_async_copy(w_rest.at[:, :, inner], wr.at[:, :, :, :, lanes], wt_sem.at[2, out_col, 0]))
            for side in PAIR:
                if first:
                    copies.append(pltpu.make_async_copy(w_first.at[:, 2 * side], wfs.at[side, rows_at, :, lanes], wt_sem.at[0, out_col, 1 + side]))
                else:
                    copies.append(pltpu.make_async_copy(w_rest.at[:, :, 2 * side], wrs.at[:, side, rows_at, :, lanes], wt_sem.at[2, out_col, 1 + side]))
        return copies

    for copy in weight_copies(True):
        copy.start()

    blank = jnp.zeros((3, LANES), F32)
    blocks = []
    for row_off in range(3):
        parts = []
        for col_off in range(4):
            taps = [w_out[row_off, col_off - out_col].astype(F32) if 0 <= col_off - out_col < 3 else blank for out_col in PAIR]
            parts.append(jnp.concatenate(taps + [blank[0:2]], axis=0))
        blocks.append(jnp.concatenate(parts, axis=1))
    blocks.append(jnp.zeros_like(blocks[0]))
    wo[...] = jnp.concatenate(blocks, axis=0).astype(BF16)

    def load_group(g, carry):
        def body(chunk, sums):
            sum_one, sum_two = sums
            index = g * CHUNKS + chunk
            slot = lax.rem(index, DEPTH)
            for half in PAIR:
                input_copy(g, chunk, half).wait()
            for line in range(CHUNK):
                tile = stage[slot, :, :, line].reshape(WIDE, WIDE)
                out = jnp.dot(perm[...], tile, preferred_element_type=F32)
                cube = out.reshape(SUB, SUB, WIDE)
                sum_one = sum_one + jnp.sum(cube, axis=0)
                sum_two = sum_two + jnp.sum(cube * cube, axis=0)
                raw_a[g, chunk * CHUNK + line] = out.astype(BF16).reshape(8, 2, SUB, WIDE)
            later = index + DEPTH

            @pl.when(later < 2 * CHUNKS)
            def _():
                next_g = later // CHUNKS
                for half in PAIR:
                    input_copy(next_g, later - next_g * CHUNKS, half).start()

            @pl.when(index == 1)
            def _():
                pl.semaphore_wait(barrier, around)
                if rounds > 1:
                    greet(ready.at[0])

            for later_round in range(1, rounds):
                @pl.when(index == 1 + 4 * later_round)
                def _():
                    pl.semaphore_wait(ready.at[later_round - 1], around)
                    if later_round < rounds - 1:
                        greet(ready.at[later_round])

            @pl.when(chunk > 0)
            def _():
                send_cols(raw_a, col_a, 0, g, (chunk - 1) * CHUNK, CHUNK)

            return sum_one, sum_two

        zero = jnp.zeros((SUB, WIDE), F32)
        sum_one, sum_two = lax.fori_loop(0, CHUNKS, body, (zero, zero))
        send_sums(0, g, message_of(sum_one, sum_two, sum_a[...]))
        send_cols(raw_a, col_a, 0, g, SLAB - CHUNK, CHUNK)
        send_ends(raw_a, row_a, cor_a, 0, g)
        return carry

    over_groups(load_group)
    for copy in weight_copies(False):
        copy.start()
    for copy in weight_copies(True):
        copy.wait()

    def bias_row(index):
        return bias_f[pl.ds(index, 1)]

    def first_conv(g, carry):
        finish_exchange(raw_a, col_a, row_a, cor_a, 0, g)
        scale, shift = half_affine(0, g, cast_a[...], norm_first[...], WIDE)
        chunk = activation(raw_a, act_a, col_a, row_a, cor_a, 0, g, scale, shift)
        convolve(act_a, chunk, WIDE, lambda: (wf[...].reshape(1536, WIDE), wfs[0].reshape(DEEP, WIDE), wfs[1].reshape(DEEP, WIDE)), bias_row(0), raw_t, col_t, row_t, cor_t, 1, g)
        return carry

    over_groups(first_conv)
    for copy in weight_copies(False):
        copy.wait()

    def layer(src, norm_at, weights, bias, dst, par, g, **more):
        finish_exchange(src, col_t, row_t, cor_t, par, g)
        scale, shift = half_affine(par, g, cast_t[...], norm_rest[norm_at], LANES)
        chunk = activation(src, act_t, col_t, row_t, cor_t, par, g, scale, shift)
        if weights is not None:
            convolve(act_t, chunk, LANES, weights, bias, dst, col_t, row_t, cor_t, 1 - par, g, **more)
        return chunk

    def side_weights(index):
        return wrs[index, 0].reshape(SIDE, WIDE), wrs[index, 1].reshape(SIDE, WIDE)

    def shortcut_conv(g, carry):
        def extra(span):
            return [raw_a[g, span, :, which].reshape(BLOCK * LANES, WIDE) for which in range(2)]

        def weights():
            return (jnp.concatenate([wr[0].reshape(768, WIDE), ws[...].reshape(SIDE, WIDE)], axis=0), *side_weights(0))

        layer(raw_t, 0, weights, bias_row(1) + bias_row(6), raw_h, 1, g, extra=extra)
        return carry

    over_groups(shortcut_conv)

    def resnet(res, carry):
        base = 2 * res + 1

        def first_half(g, inner):
            layer(raw_h, base, lambda: (wr[base].reshape(768, WIDE), *side_weights(base)), bias_row(base + 1), raw_t, 0, g)
            return inner

        def second_half(g, inner):
            layer(raw_t, base + 1, lambda: (wr[base + 1].reshape(768, WIDE), *side_weights(base + 1)), bias_row(base + 2), raw_h, 1, g, residual=raw_h)
            return inner

        over_groups(first_half)
        over_groups(second_half)
        return carry

    over_groups(resnet)

    def out_conv(g, carry):
        chunk = layer(raw_h, 5, None, None, None, 0, g)
        sums = {}

        def products(ring, local, first):
            taps = [ring[local:BLOCK, col_off // 2:col_off // 2 + 8, col_off % 2].reshape((BLOCK - local) * LANES, LANES) for col_off in range(4)]
            out = lax.dot_general(wo[...], jnp.concatenate(taps, axis=1), (((1,), (1,)), ((), ())), preferred_element_type=F32)
            for line in range(BLOCK - local):
                sums[first + line] = out[:, line * LANES:(line + 1) * LANES]

        chunk(-1)
        products(act_t[2], BLOCK - 2, 0)
        chunk(0)
        for step in range(STEPS):
            chunk(step + 1)
            products(act_t[step % 3], 0, step * BLOCK + 2)
            for line in range(step * BLOCK, step * BLOCK + BLOCK):
                flat[pl.ds(line, 8, stride=SLAB), :] = sums[line][0:8] + sums[line + 1][8:SUB] + sums[line + 2][SUB:SUB + 8]
        for channel in range(3):
            lines = [flat[pl.ds((3 * out_col + channel) * SLAB, SLAB), :] for out_col in PAIR]
            values = jnp.concatenate(lines, axis=1)
            total = jnp.zeros((LANES, 2 * SLAB), F32)
            for _ in range(3):
                term = values.astype(BF16)
                values = values - term.astype(F32)
                blank_half = jnp.zeros_like(term)
                spread = jnp.concatenate([jnp.concatenate([term, blank_half], axis=1), jnp.concatenate([blank_half, term], axis=1)], axis=0)
                total = total + lax.dot_general(order[...], spread, (((1,), (1,)), ((), ())), preferred_element_type=F32)
            image[pl.ds(g * 8, 8), channel] = total.reshape(8, SUB, 2 * SLAB)
        return carry

    over_groups(out_conv)


def solution(mesh):
    rows_n = mesh.shape["sy"]
    cols_n = mesh.shape["sx"]
    tile_spec = P("dp", "sy", "sx", None)
    replicated = P()
    dma = pltpu.SemaphoreType.DMA

    def local_decode(act_in, norm_first, w_first, w_short, norm_rest, w_rest, bias_rest, w_out, bias_out):
        vmem = pl.BlockSpec(memory_space=pltpu.VMEM)
        anywhere = pl.BlockSpec(memory_space=pl.ANY)
        planes = pl.pallas_call(
            functools.partial(kernel, rows_n, cols_n),
            out_shape=jax.ShapeDtypeStruct((SUB, 3, SUB, 2 * SLAB), F32),
            in_specs=[anywhere, vmem, anywhere, anywhere, vmem, anywhere, vmem, vmem],
            out_specs=vmem,
            scratch_shapes=[
                pltpu.VMEM((8 * SLAB, LANES), F32),
                pltpu.VMEM((LANES, 2 * WIDE), BF16),
                pltpu.VMEM((8, LANES), F32),
                pltpu.VMEM((DEPTH, 2, 8, CHUNK, SUB, WIDE), BF16),
                pltpu.VMEM((2, SLAB, 8, 2, SUB, WIDE), BF16),
                pltpu.VMEM((2, SLAB, 8, 2, SUB, LANES), BF16),
                pltpu.VMEM((2, SLAB, 8, 2, SUB, LANES), BF16),
                *[pltpu.VMEM((BLOCK, 9, 2, SUB, WIDE), BF16)] * 3,
                *[pltpu.VMEM((BLOCK, 9, 2, SUB, LANES), BF16)] * 3,
                pltpu.VMEM((3, 2, WIDE, WIDE), BF16),
                pltpu.VMEM((2, 4, WIDE, WIDE), BF16),
                pltpu.VMEM((2, WIDE, WIDE), BF16),
                pltpu.VMEM((5, 3, 2, LANES, WIDE), BF16),
                pltpu.VMEM((5, 2, 4, LANES, WIDE), BF16),
                pltpu.VMEM((32, 4 * LANES), BF16),
                pltpu.VMEM((WIDE, WIDE), BF16),
                pltpu.VMEM((SIDE, LANES), BF16),
                pltpu.VMEM((WIDE, LANES), BF16),
                pltpu.VMEM((LANES, SIDE), BF16),
                pltpu.VMEM((LANES, WIDE), BF16),
                pltpu.VMEM((1, 2, 2, SLAB, SUB, WIDE), BF16),
                pltpu.VMEM((1, 2, 2, 8, 2, SUB, WIDE), BF16),
                pltpu.VMEM((1, 2, 2, 2, SUB, WIDE), BF16),
                pltpu.VMEM((2, 2, 2, SLAB, SUB, LANES), BF16),
                pltpu.VMEM((2, 2, 2, 8, 2, SUB, LANES), BF16),
                pltpu.VMEM((2, 2, 2, 2, SUB, LANES), BF16),
                pltpu.VMEM((2, 2, rows_n * cols_n, 8, LANES), F32),
                dma((DEPTH, 2)),
                dma((3, 2, 3)),
                dma((2, 2, 2)),
                dma((2, 2, 2)),
                dma((2, 2, 2)),
                dma((2, 2, 2)),
                dma((2, 2, 2, 2)),
                dma((2, 2, 2, 2)),
                dma((2, 2)),
                dma((2, 2)),
                pltpu.SemaphoreType.REGULAR((max(rows_n, cols_n),)),
            ],
            compiler_params=pltpu.CompilerParams(collective_id=0, has_side_effects=True, vmem_limit_bytes=62 << 20),
            name="decode",
        )(act_in, norm_first, w_first, w_short, norm_rest, w_rest, bias_rest, jnp.transpose(w_out, (0, 1, 3, 2)))
        return jnp.transpose(planes, (0, 3, 2, 1)) + bias_out.astype(F32)

    return jax.shard_map(local_decode, mesh=mesh, in_specs=(tile_spec, replicated, replicated, replicated, replicated, replicated, replicated, replicated, replicated), out_specs=tile_spec, check_vma=False)
```
